8 devices in a mesh: ez: 2 (over z, y), ey: 2 (over x), ex: 2 (over core).
Axes of the slice: x: 2, y: 2, z: 1, core: 2. Of those that a mesh axis runs over, the one named last changes fastest.
Arguments:
- tokens: bfloat16 [2048, 2048], P(('ez', 'ey', 'ex'))
- expert_ids: int32 [2048, 6], P(('ez', 'ey', 'ex'))
- gate_weights: float32 [2048, 6], P(('ez', 'ey', 'ex'))
- w_gate: bfloat16 [64, 2048, 1408], P(('ez', 'ey', 'ex'))
- w_up: bfloat16 [64, 2048, 1408], P(('ez', 'ey', 'ex'))
- w_down: bfloat16 [64, 1408, 2048], P(('ez', 'ey', 'ex'))
Outputs:
- output: bfloat16 [2048, 2048], P(('ez', 'ey', 'ex'))
All inputs are finite; a program needn't handle non-finite values.
Results may differ from the reference program's by a relative error of at most 0.00619725.
Values are sent between devices in bfloat16 or wider.
A program may use at most 1 GiB of HBM per device.

```python
import jax
import jax.numpy as jnp
from jax import lax

HIDDEN = 2048
EXPERT_FF = 1408
EXPERTS = 64
TOP_K = 6
TOKENS = 256
DEVICES = 8
TOTAL_TOK = DEVICES * TOKENS
LOCAL_EXPERTS = EXPERTS // DEVICES
PER_EXPERT = TOTAL_TOK * TOP_K // EXPERTS


def draw_routing(route_key):
    def one_source(src_key):
        key_first, key_rest, key_dev, key_order = jax.random.split(src_key, 4)
        first_block = jax.random.permutation(key_first, LOCAL_EXPERTS)
        rest_block = jax.random.permutation(key_rest, EXPERTS - LOCAL_EXPERTS) + LOCAL_EXPERTS
        positions = jnp.arange(EXPERTS)
        spaced = positions % DEVICES == 0
        first_idx = jnp.clip(positions // DEVICES, 0, LOCAL_EXPERTS - 1)
        rest_idx = jnp.clip(positions - positions // DEVICES - 1, 0, EXPERTS - LOCAL_EXPERTS - 1)
        expert_cycle = jnp.where(spaced, first_block[first_idx], rest_block[rest_idx])
        dev_perm = jax.random.permutation(key_dev, DEVICES)
        expert_cycle = dev_perm[expert_cycle // LOCAL_EXPERTS] * LOCAL_EXPERTS + expert_cycle % LOCAL_EXPERTS
        tok_perm = jax.random.permutation(key_order, TOKENS)
        slot_pos = tok_perm[:, None] * TOP_K + jnp.arange(TOP_K)[None, :]
        return expert_cycle[slot_pos % EXPERTS]
    src_keys = jax.random.split(route_key, DEVICES)
    return jax.vmap(one_source)(src_keys).reshape(TOTAL_TOK, TOP_K).astype(jnp.int32)


def setup_inputs(seed: int = 0) -> dict:
    root_key = jax.random.key(seed)
    key_tok, key_ids, key_gate, key_w1, key_w3, key_w2 = jax.random.split(root_key, 6)
    tokens = jax.random.normal(key_tok, (TOTAL_TOK, HIDDEN), jnp.float32).astype(jnp.bfloat16)
    expert_ids = draw_routing(key_ids)
    gate_logits = 0.7 * jax.random.normal(key_gate, (TOTAL_TOK, TOP_K), jnp.float32)
    gate_weights = jax.nn.softmax(gate_logits, axis=-1)
    w_gate = (jax.random.normal(key_w1, (EXPERTS, HIDDEN, EXPERT_FF), jnp.float32) * HIDDEN ** -0.5).astype(jnp.bfloat16)
    w_up = (jax.random.normal(key_w3, (EXPERTS, HIDDEN, EXPERT_FF), jnp.float32) * HIDDEN ** -0.5).astype(jnp.bfloat16)
    w_down = (jax.random.normal(key_w2, (EXPERTS, EXPERT_FF, HIDDEN), jnp.float32) * (2.0 * EXPERT_FF ** -0.5)).astype(jnp.bfloat16)
    return {"tokens": tokens, "expert_ids": expert_ids, "gate_weights": gate_weights, "w_gate": w_gate, "w_up": w_up, "w_down": w_down}


def reference(tokens, expert_ids, gate_weights, w_gate, w_up, w_down):
    sort_order = jnp.argsort(expert_ids.reshape(-1), stable=True)
    rows_by_expert = (sort_order // TOP_K).reshape(EXPERTS, PER_EXPERT)
    gates_by_expert = gate_weights.reshape(-1)[sort_order].reshape(EXPERTS, PER_EXPERT)

    def expert_step(acc_out, expert_args):
        row_ids, row_gates, gate_mat, up_mat, down_mat = expert_args
        x_rows = tokens[row_ids]
        gate_act = jnp.dot(x_rows, gate_mat, preferred_element_type=jnp.float32)
        up_act = jnp.dot(x_rows, up_mat, preferred_element_type=jnp.float32)
        hidden_act = (jax.nn.silu(gate_act) * up_act).astype(jnp.bfloat16)
        expert_out = jnp.dot(hidden_act, down_mat, preferred_element_type=jnp.float32)
        acc_out = acc_out.at[row_ids].add(expert_out * row_gates[:, None])
        return acc_out, None

    init_acc = jnp.zeros((TOTAL_TOK, HIDDEN), jnp.float32)
    moe_sum = lax.scan(expert_step, init_acc, (rows_by_expert, gates_by_expert, w_gate, w_up, w_down))[0]
    return (tokens.astype(jnp.float32) + moe_sum).astype(jnp.bfloat16)
```

```python
import functools
import math

import jax
import jax.numpy as jnp
from jax import lax
from jax.experimental import pallas as pl
from jax.experimental.pallas import tpu as pltpu
from jax.sharding import PartitionSpec as P

MESH = pl.DeviceIdType.MESH
F32 = jnp.float32
BF16 = jnp.bfloat16
RING = 4
RING2 = 2
CSUB = 4
HSUB = 8


def moe_kernel(dims, x_hbm, ids_hbm, gts_hbm, w1_hbm, w3_hbm, w2_hbm, y_hbm,
               xall, ids_all, gts_all, chosen_pos, pos_col, gate_tab, tok_tab, row_tab, gcol, xg, acc, hid, ring, ring2,
               psend, drecv, qsend, lrecv, ybuf, tok_sm, row_sm,
               loc_sem, tab_sem, rsend, rrecv, asend, arecv, wsem, w2sem, dsend, drsem, lsend, lrsem, ysem):
    tok, hidden, ff, n_loc, per_exp, topk = dims
    nc = hidden // (CSUB * 128)
    kc = CSUB * 128
    nh = hidden // (HSUB * 128)
    hc = HSUB * 128
    half = tok // 2
    n_dev = 8
    ct_ff = ff // 128
    zero_row = n_loc * per_exp
    xs = per_exp + 8

    z, y, c = lax.axis_index("ez"), lax.axis_index("ey"), lax.axis_index("ex")
    me = z * 4 + y * 2 + c
    xn, yn, pn = (z, 1 - y, c), (1 - z, y, c), (z, y, 1 - c)
    i_x = z * 4 + (1 - y) * 2 + c
    i_y = (1 - z) * 4 + y * 2 + c
    i_d = (1 - z) * 4 + (1 - y) * 2 + c

    def flip(i):
        b2, b1, b0 = (i >> 2) & 1, (i >> 1) & 1, i & 1
        t = (1 - z if b2 else z, 1 - y if b1 else y, 1 - c if b0 else c)
        return t, t[0] * 4 + t[1] * 2 + t[2]

    def w13_copies(k, e, slot):
        rows = pl.ds(k * kc, kc)
        return (pltpu.make_async_copy(w1_hbm.at[e, rows, :], ring.at[slot, 0], wsem.at[slot, 0]),
                pltpu.make_async_copy(w3_hbm.at[e, rows, :], ring.at[slot, 1], wsem.at[slot, 1]))

    def w2_copy(h, e, slot):
        return pltpu.make_async_copy(w2_hbm.at[e, :, pl.ds(h * hc, hc)], ring2.at[slot], w2sem.at[slot])

    own = pl.ds(pl.multiple_of(me * tok, tok), tok)
    loc = [pltpu.make_async_copy(x_hbm.at[k], xall[k].at[own], loc_sem.at[k]) for k in range(nc)]
    rlocs = [pltpu.make_async_copy(ids_hbm, ids_all.at[me], tab_sem.at[0]),
             pltpu.make_async_copy(gts_hbm, gts_all.at[me], tab_sem.at[3])]
    for cp in rlocs:
        cp.start()
    for cp in loc:
        cp.start()
    barrier = pltpu.get_barrier_semaphore()
    for i in range(1, n_dev):
        pl.semaphore_signal(barrier, inc=1, device_id=flip(i)[0], device_id_type=MESH)
    for e in range(RING):
        for cp in w13_copies(0, e, e):
            cp.start()
    pl.semaphore_wait(barrier, n_dev - 1)

    for cp in rlocs:
        cp.wait()
    rcopies = []
    for i in range(1, n_dev):
        for q, ref in enumerate((ids_all, gts_all)):
            cp = pltpu.make_async_remote_copy(ref.at[me], ref.at[me], rsend.at[q, i - 1], rrecv.at[q, i - 1],
                                              device_id=flip(i)[0], device_id_type=MESH)
            cp.start()
            rcopies.append(cp)

    def region(k, dev, lo, n):
        return xall[k].at[pl.ds(pl.multiple_of(dev * tok + lo, half), n)]

    partner_of = lambda d: d + 1 - 2 * c
    i_p = partner_of(me)
    flows = [
        (xn, me, i_x, 0, half), (xn, me, i_x, half, half), (xn, i_y, i_d, half, half),
        (yn, me, i_y, half, half), (yn, me, i_y, 0, half), (yn, i_x, i_d, 0, half),
        (pn, me, i_p, 0, tok),
        (pn, i_x, partner_of(i_x), 0, half), (pn, i_x, partner_of(i_x), half, half),
        (pn, i_y, partner_of(i_y), half, half), (pn, i_y, partner_of(i_y), 0, half),
        (pn, i_d, partner_of(i_d), 0, half), (pn, i_d, partner_of(i_d), half, half),
    ]

    def ag(k, n):
        tgt, src, _, lo, rows = flows[n]
        return pltpu.make_async_remote_copy(region(k, src, lo, rows), region(k, src, lo, rows),
                                            asend.at[k, n], arecv.at[k, n], device_id=tgt, device_id_type=MESH)

    def ag_recv(k, n):
        tgt, _, src, lo, rows = flows[n]
        pltpu.make_async_remote_copy(region(k, src, lo, rows), region(k, src, lo, rows),
                                     asend.at[k, n], arecv.at[k, n], device_id=tgt, device_id_type=MESH).wait_recv()

    def own_sends(k):
        for n in (0, 3, 1, 4, 6):
            ag(k, n).start()

    def relay1(k):
        ag_recv(k, 0)
        ag(k, 5).start()
        ag(k, 7).start()
        ag_recv(k, 3)
        ag(k, 2).start()
        ag(k, 9).start()

    def relay2(k):
        ag_recv(k, 1)
        ag(k, 8).start()
        ag_recv(k, 4)
        ag(k, 10).start()

    def relay3(k):
        ag_recv(k, 5)
        ag(k, 11).start()
        ag_recv(k, 2)
        ag(k, 12).start()

    def finish(k):
        for n in (6, 7, 9, 8, 10, 11, 12):
            ag_recv(k, n)

    for k in range(2):
        loc[k].wait()
        own_sends(k)
    for k in range(2, nc):
        loc[k].wait()

    for cp in rcopies:
        cp.wait()
    base = me * n_loc
    my_ids = lax.broadcasted_iota(jnp.int32, (n_loc, tok), 0) + base
    off = jnp.zeros((n_loc, 1), jnp.int32)
    for s in range(n_dev):
        ids_s = ids_all[s]
        gts_s = gts_all[s]
        hit = jnp.zeros((n_loc, tok), jnp.int32)
        gden = jnp.zeros((n_loc, tok), F32)
        for j in range(topk):
            m = ids_s[j:j + 1, :] == my_ids
            hit = jnp.where(m, 1, hit)
            gden = gden + jnp.where(m, gts_s[j:j + 1, :], 0.0)
        cum = hit
        step = 1
        while step < tok:
            cum = cum + jnp.concatenate([jnp.zeros((n_loc, step), jnp.int32), cum[:, 0:tok - step]], axis=1)
            step *= 2
        pos = off + cum - 1
        off = off + cum[:, tok - 1:tok]
        posm = jnp.where(hit > 0, pos, -1)
        chosen_pos[0:n_loc, s * tok:(s + 1) * tok] = posm
        gate_tab[0:n_loc, s * tok:(s + 1) * tok] = gden
        rows = jnp.full((8, tok), zero_row, jnp.int32)
        for e in range(n_loc):
            rows = jnp.where(ids_s == base + e, e * per_exp + pos[e:e + 1, :], rows)
        row_tab[:, s * tok:(s + 1) * tok] = rows
        pos_col[s * tok:(s + 1) * tok, 0:n_loc] = posm.T
    row_cp = pltpu.make_async_copy(row_tab, row_sm, tab_sem.at[1])
    row_cp.start()

    ipos = lax.broadcasted_iota(jnp.int32, (per_exp, tok), 0)
    lpos = lax.broadcasted_iota(jnp.int32, (tok, per_exp), 1)
    tcol = lax.broadcasted_iota(jnp.int32, (tok, per_exp), 0)
    for e in range(n_loc):
        def tok_step(s, tsum, e=e):
            pc = pos_col[pl.ds(pl.multiple_of(s * tok, tok), tok), e:e + 1]
            return tsum + jnp.where(pc == lpos, tcol + s * tok, 0)

        tsum = lax.fori_loop(0, n_dev, tok_step, jnp.zeros((tok, per_exp), jnp.int32))
        tok_tab[e:e + 1, 0:per_exp] = jnp.sum(tsum, axis=0, keepdims=True)

    def table_step(e, carry):
        gsum = jnp.zeros((per_exp, tok), F32)
        for s in range(n_dev):
            prow = chosen_pos[pl.ds(e, 1), s * tok:(s + 1) * tok]
            grow = gate_tab[pl.ds(e, 1), s * tok:(s + 1) * tok]
            gsum = gsum + jnp.where(prow == ipos, grow, 0.0)
        gcol[e] = jnp.broadcast_to(jnp.sum(gsum, axis=1, keepdims=True), (per_exp, 128))
        return carry

    lax.fori_loop(0, n_loc, table_step, 0)
    tok_cp = pltpu.make_async_copy(tok_tab.at[0:n_loc], tok_sm, tab_sem.at[2])
    tok_cp.start()

    relay1(0)
    relay2(0)
    if nc > 2:
        own_sends(2)
    row_cp.wait()
    tok_cp.wait()
    relay3(0)
    finish(0)

    def acc_row(e, mat, ct):
        return ((e * 2 + mat) * ct_ff + ct) * (per_exp // 8)

    def proj_step(k, e):
        slot = lax.rem(e, RING)

        def pick(i, carry):
            for u in range(8):
                r = i * 8 + u
                xg[pl.ds(r, CSUB, stride=xs), :] = xall[k][tok_sm[e, r]].astype(F32)
            return carry

        lax.fori_loop(0, per_exp // 8, pick, 0)
        for cp in w13_copies(k, e, slot):
            cp.wait()
        xe = jnp.concatenate([xg[ct * xs:ct * xs + per_exp, :] for ct in range(CSUB)], axis=1).astype(BF16)
        for ct in range(0, ct_ff, 2):
            w = min(2, ct_ff - ct)
            cols = slice(ct * 128, (ct + w) * 128)
            if w == 2:
                d = [jnp.dot(xe, ring[slot, mat, :, cols], preferred_element_type=F32) for mat in range(2)]
            else:
                both = jnp.concatenate([ring[slot, 0, :, cols], ring[slot, 1, :, cols]], axis=1)
                r = jnp.dot(xe, both, preferred_element_type=F32)
                d = [r[:, 0:128], r[:, 128:256]]
            for q in range(w):
                parts = []
                for mat in range(2):
                    at = pl.ds(acc_row(e, mat, ct + q), per_exp // 8)
                    v = d[mat][:, q * 128:(q + 1) * 128]
                    if k > 0:
                        v = v + acc[at].reshape(per_exp, 128)
                    if k < nc - 1:
                        acc[at] = v.reshape(per_exp // 8, 8, 128)
                    parts.append(v)
                if k == nc - 1:
                    hid[e, :, (ct + q) * 128:(ct + q + 1) * 128] = (jax.nn.silu(parts[0]) * parts[1]).astype(BF16)
        if k < nc - 1:
            @pl.when(e < n_loc - RING)
            def _():
                for cp in w13_copies(k, e + RING, slot):
                    cp.start()

            @pl.when(e >= n_loc - RING)
            def _():
                for cp in w13_copies(k + 1, e + RING - n_loc, slot):
                    cp.start()
        else:
            @pl.when(e < n_loc - RING)
            def _():
                for cp in w13_copies(k, e + RING, slot):
                    cp.start()

    for k in range(nc):
        if k == nc - 1:
            for e in range(RING2):
                w2_copy(0, e, e).start()

        def body(e, carry, k=k):
            proj_step(k, e)
            if k + 1 < nc:
                @pl.when(e == 1)
                def _():
                    relay1(k + 1)
                    relay2(k + 1)
                    if k + 3 < nc:
                        own_sends(k + 3)

                @pl.when(e == 5)
                def _():
                    relay3(k + 1)
            return carry

        lax.fori_loop(0, n_loc, body, 0)
        if k + 1 < nc:
            finish(k + 1)

    flat = acc.reshape(acc.shape[0] * 8, 128)

    def down(h):
        def body(e, carry):
            slot = lax.rem(e, RING2)
            w2_copy(h, e, slot).wait()
            g = gcol[e]
            for n in range(0, HSUB, 2):
                o = jnp.dot(hid[e], ring2[slot, :, n * 128:(n + 2) * 128], preferred_element_type=F32)
                for q in range(2):
                    flat[pl.ds(e * (per_exp * HSUB) + n + q, per_exp, stride=HSUB), :] = o[:, q * 128:(q + 1) * 128] * g

            @pl.when(e < n_loc - RING2)
            def _():
                w2_copy(h, e + RING2, slot).start()

            if h + 1 < nh:
                @pl.when(e >= n_loc - RING2)
                def _():
                    w2_copy(h + 1, e + RING2 - n_loc, slot).start()
            return carry

        lax.fori_loop(0, n_loc, body, 0)

    def token_sum(t):
        v = None
        for j in range(topk):
            r = acc[row_sm[j, t]]
            v = r if v is None else v + r
        return v

    def pair_sum(t):
        return jnp.concatenate([token_sum(t), token_sum(t + 1)], axis=0)

    pr = 2 * HSUB

    def each_pair(lo, n, fn):
        def body(i, carry):
            for u in range(2):
                fn(i * 2 + u)
            return carry
        lax.fori_loop(lo // 4, (lo + n) // 4, body, 0)

    def at_pair(i):
        return pl.ds(pl.multiple_of(i * pr, pr), pr)

    f_base = zero_row + 8
    qx_base = lambda h: f_base + h * half * 4
    qy_base = lambda h: qx_base(h) + half
    yo_base = lambda h: qx_base(h) + 2 * half

    def d2d(h, g):
        return pltpu.make_async_remote_copy(psend.at[h, g], drecv.at[h, g], dsend.at[h, g], drsem.at[h, g],
                                            device_id=pn, device_id_type=MESH)

    def link(h, n):
        return pltpu.make_async_remote_copy(qsend.at[h, n], lrecv.at[h, n], lsend.at[h, n], lrsem.at[h, n],
                                            device_id=xn if n in (0, 2, 4) else yn, device_id_type=MESH)

    groups = [i_d, i_x, i_y, me]

    def partner_group(h, g):
        t0 = partner_of(groups[g]) * tok

        def fn(i):
            psend[h, g, at_pair(i), :] = pair_sum(t0 + i * 2).astype(BF16)

        each_pair(0, tok, fn)
        d2d(h, g).start()

    def plane_sum(h, g, i):
        return pair_sum(groups[g] * tok + i * 2) + drecv[h, g, at_pair(i), :].astype(F32)

    def send_part(h, g, lo, n):
        def fn(i):
            qsend[h, n, at_pair(i - lo // 2), :] = plane_sum(h, g, i).astype(BF16)

        each_pair(lo, half, fn)
        link(h, n).start()

    def keep_part(h, g, lo, n, base):
        def fn(i):
            acc[pl.ds(base + i * 2 - lo, 2)] = plane_sum(h, g, i).reshape(2, HSUB, 128)

        each_pair(lo, n, fn)

    def relay_part(h, n, rn, base):
        link(h, rn).wait_recv()

        def fn(i):
            v = acc[pl.ds(base + i * 2, 2)].reshape(pr, 128)
            qsend[h, n, at_pair(i), :] = (v + lrecv[h, rn, at_pair(i), :].astype(F32)).astype(BF16)

        each_pair(0, half, fn)
        link(h, n).start()

    def combine_send(h):
        partner_group(h, 0)
        partner_group(h, 1)
        d2d(h, 0).wait_recv()
        send_part(h, 0, 0, 0)
        send_part(h, 0, half, 1)
        partner_group(h, 2)
        d2d(h, 1).wait_recv()
        send_part(h, 1, 0, 2)
        d2d(h, 2).wait_recv()
        send_part(h, 2, half, 3)
        keep_part(h, 1, half, half, qx_base(h))
        keep_part(h, 2, 0, half, qy_base(h))
        partner_group(h, 3)
        d2d(h, 3).wait_recv()
        keep_part(h, 3, 0, tok, yo_base(h))

    def combine_relay(h):
        relay_part(h, 4, 1, qx_base(h))
        relay_part(h, 5, 0, qy_base(h))

    def final(h):
        for n in (2, 3, 4, 5):
            link(h, n).wait_recv()
        for lo, n1, n2 in ((0, 2, 5), (half, 3, 4)):
            def fn(i, lo=lo, n1=n1, n2=n2):
                v = acc[pl.ds(yo_base(h) + i * 2 + lo, 2)].reshape(pr, 128)
                v = v + lrecv[h, n1, at_pair(i), :].astype(F32) + lrecv[h, n2, at_pair(i), :].astype(F32)
                for q in range(2):
                    t = (i * 2 + q) + lo
                    xr = jnp.concatenate([xall[h * (HSUB // CSUB) + m][me * tok + t] for m in range(HSUB // CSUB)], axis=0).astype(F32)
                    ybuf[t, h * HSUB:(h + 1) * HSUB, :] = (v[q * HSUB:(q + 1) * HSUB, :] + xr).astype(BF16)

            each_pair(0, half, fn)

    acc[zero_row] = jnp.zeros((HSUB, 128), F32)
    for h in range(nh):
        down(h)
        if h > 0:
            combine_relay(h - 1)
        combine_send(h)
    combine_relay(nh - 1)
    for h in range(nh):
        final(h)
    out = pltpu.make_async_copy(ybuf.at[0:tok], y_hbm, ysem.at[0])
    out.start()
    for k in range(nc):
        for n in range(13):
            ag(k, n).wait_send()
    for h in range(nh):
        for g in range(4):
            d2d(h, g).wait_send()
        for n in range(6):
            link(h, n).wait_send()
    out.wait()


def solution(mesh):
    ep_axes = tuple(mesh.axis_names)
    n_dev = math.prod(mesh.shape[a] for a in ep_axes)
    row_spec = P(ep_axes, None)
    w_spec = P(ep_axes, None, None)

    def local_layer(tokens, expert_ids, gate_weights, w_gate, w_up, w_down):
        tok, hidden = tokens.shape
        topk = expert_ids.shape[1]
        n_loc, _, ff = w_gate.shape
        per_exp = n_dev * tok * topk // (n_dev * n_loc)
        kc, hc = CSUB * 128, HSUB * 128
        nc, nh = hidden // kc, hidden // hc
        n_tok = n_dev * tok
        xt = tokens.reshape(tok, nc, CSUB, 128).transpose(1, 0, 2, 3)
        pad = ((0, 8 - topk), (0, 0))
        ids_t = jnp.pad(expert_ids.T, pad, constant_values=-1)
        gts_t = jnp.pad(gate_weights.T, pad)
        half = tok // 2
        acc_rows = max(2 * n_loc * per_exp * (ff // 128), (n_loc * per_exp + 8) * HSUB + nh * 4 * half * HSUB)
        dims = (tok, hidden, ff, n_loc, per_exp, topk)
        scratch = [
            [pltpu.VMEM((n_tok + 8, CSUB, 128), BF16) for _ in range(nc)],
            pltpu.VMEM((n_dev, 8, tok), jnp.int32),
            pltpu.VMEM((n_dev, 8, tok), F32),
            pltpu.VMEM((n_loc + 8, n_tok), jnp.int32),
            pltpu.VMEM((n_tok, 128), jnp.int32),
            pltpu.VMEM((n_loc + 8, n_tok), F32),
            pltpu.VMEM((n_loc + 8, 256), jnp.int32),
            pltpu.VMEM((8, n_tok), jnp.int32),
            pltpu.VMEM((n_loc, per_exp, 128), F32),
            pltpu.VMEM((8 * (per_exp + 8), 128), F32),
            pltpu.VMEM((acc_rows // 8, 8, 128), F32),
            pltpu.VMEM((n_loc, per_exp, ff), BF16),
            pltpu.VMEM((RING, 2, kc, ff), BF16),
            pltpu.VMEM((RING2, ff, hc), BF16),
            pltpu.VMEM((nh, 4, tok * HSUB, 128), BF16),
            pltpu.VMEM((nh, 4, tok * HSUB, 128), BF16),
            pltpu.VMEM((nh, 6, half * HSUB, 128), BF16),
            pltpu.VMEM((nh, 6, half * HSUB, 128), BF16),
            pltpu.VMEM((tok + 1, hidden // 128, 128), BF16),
            pltpu.SMEM((n_loc, 256), jnp.int32),
            pltpu.SMEM((8, n_tok), jnp.int32),
            pltpu.SemaphoreType.DMA((nc,)),
            pltpu.SemaphoreType.DMA((4,)),
            pltpu.SemaphoreType.DMA((2, n_dev - 1)),
            pltpu.SemaphoreType.DMA((2, n_dev - 1)),
            pltpu.SemaphoreType.DMA((nc, 13)),
            pltpu.SemaphoreType.DMA((nc, 13)),
            pltpu.SemaphoreType.DMA((RING, 2)),
            pltpu.SemaphoreType.DMA((RING2,)),
            pltpu.SemaphoreType.DMA((nh, 4)),
            pltpu.SemaphoreType.DMA((nh, 4)),
            pltpu.SemaphoreType.DMA((nh, 6)),
            pltpu.SemaphoreType.DMA((nh, 6)),
            pltpu.SemaphoreType.DMA((1,)),
        ]
        out = pl.pallas_call(
            functools.partial(moe_kernel, dims),
            out_shape=jax.ShapeDtypeStruct((tok, hidden // 128, 128), BF16),
            in_specs=[pl.BlockSpec(memory_space=pl.ANY)] * 6,
            out_specs=pl.BlockSpec(memory_space=pl.ANY),
            scratch_shapes=scratch,
            compiler_params=pltpu.CompilerParams(collective_id=0, has_side_effects=True,
                                                 vmem_limit_bytes=67043328),
        )(xt, ids_t, gts_t, w_gate, w_up, w_down)
        return out.reshape(tok, hidden)

    return jax.shard_map(local_layer, mesh=mesh, in_specs=(row_spec, row_spec, row_spec, w_spec, w_spec, w_spec), out_specs=row_spec, check_vma=False)
```

```python
import functools
import math

import jax
import jax.numpy as jnp
from jax import lax
from jax.experimental import pallas as pl
from jax.experimental.pallas import tpu as pltpu
from jax.sharding import PartitionSpec as P

MESH = pl.DeviceIdType.MESH
F32 = jnp.float32
BF16 = jnp.bfloat16
RING = 5
CSUB = 4
HSUB = 8
TBLK = 64
TGRP = 4
UNROLL = 8


def unrolled(n, fn):
    def body(i, carry):
        fn(jnp.minimum(i, n - 1))
        return carry
    lax.fori_loop(0, n + 1, body, 0, unroll=n)


def moe_kernel(dims, x_hbm, ids_hbm, gts_hbm, w1_hbm, w3_hbm, w2_hbm, y_hbm,
               xall, ids_all, gts_all, chosen_pos, gate_tab, tok_tab, row_tab, pos_col, xg, xb, acc, hid, ring,
               psend, drecv, qsend, lrecv, ybuf, tok_sm, win_p, win_m, row_ord,
               loc_sem, tab_sem, rsend, rrecv, asend, arecv, wsem, dsend, drsem, lsend, lrsem, ysem, row_sem):
    tok, hidden, ff, n_loc, per_exp, topk = dims
    nc = hidden // (CSUB * 128)
    kc = CSUB * 128
    nh = hidden // (HSUB * 128)
    hc = HSUB * 128
    half = tok // 2
    n_dev = 8
    ct_ff = ff // 128
    zero_row = n_loc * per_exp
    xs = per_exp + 8

    z, y, c = lax.axis_index("ez"), lax.axis_index("ey"), lax.axis_index("ex")
    me = z * 4 + y * 2 + c
    xn, yn, pn = (z, 1 - y, c), (1 - z, y, c), (z, y, 1 - c)
    i_x = z * 4 + (1 - y) * 2 + c
    i_y = (1 - z) * 4 + y * 2 + c
    i_d = (1 - z) * 4 + (1 - y) * 2 + c

    def flip(i):
        b2, b1, b0 = (i >> 2) & 1, (i >> 1) & 1, i & 1
        t = (1 - z if b2 else z, 1 - y if b1 else y, 1 - c if b0 else c)
        return t, t[0] * 4 + t[1] * 2 + t[2]

    tail = ff - hc

    def w13_copies(k, e, slot):
        out = []
        for m, w in enumerate((w1_hbm, w3_hbm)):
            rows = pl.ds(k * kc, kc)
            out.append(pltpu.make_async_copy(w.at[e, rows, pl.ds(0, hc)], ring.at[slot, pl.ds(m * kc, kc), pl.ds(0, hc)], wsem.at[slot, 2 * m]))
            out.append(pltpu.make_async_copy(w.at[e, rows, pl.ds(hc, tail)], ring.at[slot, pl.ds(2 * kc, kc), pl.ds(m * tail, tail)],
                                             wsem.at[slot, 2 * m + 1]))
        return out

    def w2_copy(h, e, slot):
        return pltpu.make_async_copy(w2_hbm.at[e, :, pl.ds(pl.multiple_of(h * hc, hc), hc)], ring.at[slot, pl.ds(0, ff)],
                                     wsem.at[slot, 0])

    def weight(slot, m, ct, w):
        if ct * 128 < hc:
            return ring[slot, m * kc:(m + 1) * kc, ct * 128:(ct + w) * 128]
        c0 = m * tail + ct * 128 - hc
        return ring[slot, 2 * kc:3 * kc, c0:c0 + w * 128]

    own = pl.ds(pl.multiple_of(me * tok, tok), tok)
    loc = [pltpu.make_async_copy(x_hbm.at[pl.ds(0, tok), pl.ds(k * hc, hc)], ring.at[RING - 1, pl.ds(k * tok, tok)], loc_sem.at[k])
           for k in range(nh)]
    rlocs = [pltpu.make_async_copy(ids_hbm, ids_all.at[me], tab_sem.at[0]),
             pltpu.make_async_copy(gts_hbm, gts_all.at[me], tab_sem.at[3])]
    for cp in rlocs:
        cp.start()
    for cp in loc:
        cp.start()
    barrier = pltpu.get_barrier_semaphore()
    for i in range(1, n_dev):
        pl.semaphore_signal(barrier, inc=1, device_id=flip(i)[0], device_id_type=MESH)
    for e in range(RING - 1):
        for cp in w13_copies(0, e, e):
            cp.start()

    def own_rows(k):
        at = k * CSUB // HSUB
        for ct in range(CSUB):
            col = (k * CSUB + ct) % HSUB * 128
            xg[pl.ds(ct, tok, stride=CSUB), :] = ring[RING - 1, at * tok:(at + 1) * tok, col:col + 128].astype(F32)

        def one(t):
            xall[k][me * tok + t] = xg[pl.ds(pl.multiple_of(t * CSUB, CSUB), CSUB), :].astype(BF16)

        unrolled(tok, one)

    loc[0].wait()
    own_rows(0)
    pl.semaphore_wait(barrier, n_dev - 1)

    for cp in rlocs:
        cp.wait()
    rcopies = []
    for i in range(1, n_dev):
        for q, ref in enumerate((ids_all, gts_all)):
            cp = pltpu.make_async_remote_copy(ref.at[me], ref.at[me], rsend.at[q, i - 1], rrecv.at[q, i - 1],
                                              device_id=flip(i)[0], device_id_type=MESH)
            cp.start()
            rcopies.append(cp)

    def region(k, dev, lo, n):
        return xall[k].at[pl.ds(pl.multiple_of(dev * tok + lo, half), n)]

    partner_of = lambda d: d + 1 - 2 * c
    i_p = partner_of(me)
    flows = [
        (xn, me, i_x, 0, half), (xn, me, i_x, half, half), (xn, i_y, i_d, half, half),
        (yn, me, i_y, half, half), (yn, me, i_y, 0, half), (yn, i_x, i_d, 0, half),
        (pn, me, i_p, 0, tok),
        (pn, i_x, partner_of(i_x), 0, half), (pn, i_x, partner_of(i_x), half, half),
        (pn, i_y, partner_of(i_y), half, half), (pn, i_y, partner_of(i_y), 0, half),
        (pn, i_d, partner_of(i_d), 0, half), (pn, i_d, partner_of(i_d), half, half),
    ]

    def ag(k, n):
        tgt, src, _, lo, rows = flows[n]
        return pltpu.make_async_remote_copy(region(k, src, lo, rows), region(k, src, lo, rows),
                                            asend.at[k, n], arecv.at[k, n], device_id=tgt, device_id_type=MESH)

    def ag_recv(k, n):
        tgt, _, src, lo, rows = flows[n]
        pltpu.make_async_remote_copy(region(k, src, lo, rows), region(k, src, lo, rows),
                                     asend.at[k, n], arecv.at[k, n], device_id=tgt, device_id_type=MESH).wait_recv()

    def own_sends(k):
        for n in (0, 3, 1, 4, 6):
            ag(k, n).start()

    def relay1(k):
        ag_recv(k, 0)
        ag(k, 5).start()
        ag(k, 7).start()
        ag_recv(k, 3)
        ag(k, 2).start()
        ag(k, 9).start()

    def relay2(k):
        ag_recv(k, 1)
        ag(k, 8).start()
        ag_recv(k, 4)
        ag(k, 10).start()

    def relay3(k):
        ag_recv(k, 5)
        ag(k, 11).start()
        ag_recv(k, 2)
        ag(k, 12).start()

    def finish(k):
        for n in (6, 7, 9, 8, 10, 11, 12):
            ag_recv(k, n)

    own_sends(0)
    for k in range(1, nc):
        if k * CSUB % HSUB == 0:
            loc[k * CSUB // HSUB].wait()
        own_rows(k)
    for cp in w13_copies(0, RING - 1, RING - 1):
        cp.start()

    for cp in rcopies:
        cp.wait()
    base = me * n_loc
    my_ids = lax.broadcasted_iota(jnp.int32, (n_loc, tok), 0) + base
    off = jnp.zeros((n_loc, 1), jnp.int32)
    for s in range(n_dev):
        ids_s = ids_all[s]
        gts_s = gts_all[s]
        hit = jnp.zeros((n_loc, tok), jnp.int32)
        gden = jnp.zeros((n_loc, tok), F32)
        for j in range(topk):
            m = ids_s[j:j + 1, :] == my_ids
            hit = jnp.where(m, 1, hit)
            gden = gden + jnp.where(m, gts_s[j:j + 1, :], 0.0)
        cum = hit
        step = 1
        while step < tok:
            cum = cum + jnp.concatenate([jnp.zeros((n_loc, step), jnp.int32), cum[:, 0:tok - step]], axis=1)
            step *= 2
        pos = off + cum - 1
        off = off + cum[:, tok - 1:tok]
        posm = jnp.where(hit > 0, pos, -1)
        chosen_pos[s] = posm
        pos_col[s * tok:(s + 1) * tok, 0:n_loc] = posm.T
        gate_tab[s] = gden
        rows = jnp.full((topk, tok), zero_row, jnp.int32)
        for e in range(n_loc):
            rows = jnp.where(ids_s == base + e, e * per_exp + pos[e:e + 1, :], rows)
        for q in range(tok // 128):
            at = (s * (tok // 128) + q) * 8
            row_tab[at:at + topk, :] = rows[:, q * 128:(q + 1) * 128]
            row_tab[at + topk:at + 8, :] = jnp.zeros((8 - topk, 128), jnp.int32)
    order = [(i_d, 0), (i_d, 1), (i_x, 0), (i_y, 1), (i_x, 1), (i_y, 0), (me, 0), (me, 1)]
    n_blk = len(order)
    for b, (dev, hf) in enumerate(order):
        for side, d in enumerate((partner_of(dev), dev)):
            row_ord[side, b] = row_tab[pl.ds(pl.multiple_of((d * 2 + hf) * 8, 8), 8), :]

    def window(side, b):
        return pltpu.make_async_copy(row_ord.at[side, b], (win_p, win_m)[side], row_sem.at[side])

    relay1(0)
    own_sends(1)
    relay2(0)
    lpos = lax.broadcasted_iota(jnp.int32, (TBLK, per_exp), 1)
    tcol = lax.broadcasted_iota(jnp.int32, (TBLK, per_exp), 0)
    for e0 in range(0, n_loc, TGRP):
        def tok_step(i, sums, e0=e0):
            pc = pos_col[pl.ds(pl.multiple_of(i * TBLK, TBLK), TBLK), :]
            out = []
            for e in range(TGRP):
                hitv = jnp.where(pc[:, e0 + e:e0 + e + 1] == lpos, tcol + i * TBLK, 0)
                out.append(sums[e] + jnp.sum(hitv.reshape(TBLK // 8, 8, per_exp), axis=0))
            return tuple(out)

        sums = lax.fori_loop(0, n_dev * tok // TBLK, tok_step,
                             tuple(jnp.zeros((8, per_exp), jnp.int32) for _ in range(TGRP)))
        for e in range(TGRP):
            tok_tab[e0 + e:e0 + e + 1, 0:per_exp] = jnp.sum(sums[e], axis=0, keepdims=True)

    tok_cp = pltpu.make_async_copy(tok_tab.at[0:n_loc], tok_sm, tab_sem.at[2])
    tok_cp.start()

    relay3(0)

    tok_cp.wait()
    finish(0)

    def acc_row(e, mat, ct):
        return ((e * 2 + mat) * ct_ff + ct) * (per_exp // 8)

    def pick(k, e, lo, n):
        def one(i):
            xg[pl.ds(lo + i, CSUB, stride=xs), :] = xall[k][tok_sm[e, lo + i]].astype(F32)

        unrolled(n, one)

    def proj_step(k, e):
        slot = lax.rem(k * n_loc + e, RING)
        for cp in w13_copies(k, e, slot):
            cp.wait()
        for ct in range(CSUB):
            xb[:, ct * 128:(ct + 1) * 128] = xg[ct * xs:ct * xs + per_exp, :].astype(BF16)
        nxt = jnp.minimum(e + 1, n_loc - 1)
        steps = list(range(0, ct_ff, 2))
        share = per_exp // len(steps)
        for si, ct in enumerate(steps):
            w = min(2, ct_ff - ct)
            if w == 2:
                d = [jnp.dot(xb[...], weight(slot, mat, ct, w), preferred_element_type=F32) for mat in range(2)]
            else:
                both = jnp.concatenate([weight(slot, mat, ct, w) for mat in range(2)], axis=1)
                r = jnp.dot(xb[...], both, preferred_element_type=F32)
                d = [r[:, 0:128], r[:, 128:256]]
            pick(k, nxt, si * share, share)
            for q in range(w):
                parts = []
                for mat in range(2):
                    at = pl.ds(acc_row(e, mat, ct + q), per_exp // 8)
                    v = d[mat][:, q * 128:(q + 1) * 128]
                    if k > 0:
                        v = v + acc[at].reshape(per_exp, 128)
                    if k < nc - 1:
                        acc[at] = v.reshape(per_exp // 8, 8, 128)
                    parts.append(v)
                if k == nc - 1:
                    hid[e, :, (ct + q) * 128:(ct + q + 1) * 128] = (jax.nn.silu(parts[0]) * parts[1]).astype(BF16)
        @pl.when(e < n_loc - RING)
        def _():
            for cp in w13_copies(k, e + RING, slot):
                cp.start()

        @pl.when(e >= n_loc - RING)
        def _():
            if k < nc - 1:
                for cp in w13_copies(k + 1, e + RING - n_loc, slot):
                    cp.start()
            else:
                w2_copy(0, e + RING - n_loc, slot).start()

    for k in range(nc):
        pick(k, 0, 0, per_exp)

        def body(e, carry, k=k):
            proj_step(k, e)
            if k + 1 < nc:
                @pl.when(e == 1)
                def _():
                    relay1(k + 1)
                    if k + 2 < nc:
                        own_sends(k + 2)

                @pl.when(e == 4)
                def _():
                    relay2(k + 1)

                @pl.when(e == 6)
                def _():
                    relay3(k + 1)
            return carry

        lax.fori_loop(0, n_loc, body, 0)
        if k + 1 < nc:
            finish(k + 1)

    flat = acc.reshape(acc.shape[0] * 8, 128)

    def down(h):
        def body(e, carry):
            step = h * n_loc + e
            slot = lax.rem(nc * n_loc + step, RING)
            w2_copy(h, e, slot).wait()
            ipos = lax.broadcasted_iota(jnp.int32, (per_exp, tok), 0)
            gsum = jnp.zeros((per_exp, tok), F32)
            for s in range(n_dev):
                prow = chosen_pos[s, pl.ds(e, 1), :]
                grow = gate_tab[s, pl.ds(e, 1), :]
                gsum = gsum + jnp.where(prow == ipos, grow, 0.0)
            g = jnp.broadcast_to(jnp.sum(gsum, axis=1, keepdims=True), (per_exp, 128))
            for n in range(0, HSUB, 2):
                o = jnp.dot(hid[e], ring[slot, 0:ff, n * 128:(n + 2) * 128], preferred_element_type=F32)
                for q in range(2):
                    flat[pl.ds(e * (per_exp * HSUB) + n + q, per_exp, stride=HSUB), :] = o[:, q * 128:(q + 1) * 128] * g

            @pl.when(e < n_loc - RING)
            def _():
                w2_copy(h, e + RING, slot).start()

            @pl.when(jnp.logical_and(e >= n_loc - RING, h < nh - 1))
            def _():
                w2_copy(h + 1, e + RING - n_loc, slot).start()

            return carry

        lax.fori_loop(0, n_loc, body, 0)

    def pair_sum(win, i):
        out = []
        for t in (2 * i, 2 * i + 1):
            v = acc[win[0, t]]
            for j in range(1, topk):
                v = v + acc[win[j, t]]
            out.append(v)
        return jnp.concatenate(out, axis=0)

    pr = 2 * HSUB
    f_base = zero_row + 8

    def at_pair(i):
        return pl.ds(i * pr if isinstance(i, int) else pl.multiple_of(i * pr, pr), pr)

    def kept(h, b):
        return f_base + (h * n_blk + b) * half

    def d2d(h, b):
        return pltpu.make_async_remote_copy(psend.at[h, b], drecv.at[h, b], dsend.at[h, b], drsem.at[h, b],
                                            device_id=pn, device_id_type=MESH)

    def link(h, n):
        par = n % 2 if isinstance(n, int) else lax.rem(n, 2)
        tgt = (z + par * (1 - 2 * z), y + (1 - par) * (1 - 2 * y), c)
        return pltpu.make_async_remote_copy(qsend.at[h, n], lrecv.at[h, n], lsend.at[h, n], lrsem.at[h, n],
                                            device_id=tgt, device_id_type=MESH)

    def pairs(fn):
        def body(i, carry):
            for u in range(UNROLL):
                fn(i * UNROLL + u)
            return carry
        lax.fori_loop(0, half // (2 * UNROLL), body, 0)

    def relay_part(h, n, rn, base):
        link(h, rn).wait_recv()

        def fn(i):
            v = acc[pl.ds(base + i * 2, 2)].reshape(pr, 128)
            qsend[h, n, at_pair(i), :] = (v + lrecv[h, rn, at_pair(i), :].astype(F32)).astype(BF16)

        pairs(fn)
        link(h, n).start()

    def combine_send(h):
        def body(b, carry):
            @pl.when(b < n_blk)
            def _():
                window(0, b).wait()

                def part(i):
                    psend[h, b, at_pair(i), :] = pair_sum(win_p, i).astype(BF16)

                unrolled(half // 2, part)
                d2d(h, b).start()

                @pl.when(b < n_blk - 1)
                def _():
                    window(0, b + 1).start()

            @pl.when(b > 0)
            def _():
                m = b - 1
                d2d(h, m).wait_recv()
                window(1, m).wait()
                n = jnp.minimum(m, 5)

                def whole(i):
                    v = pair_sum(win_m, i) + drecv[h, m, at_pair(i), :].astype(F32)
                    qsend[h, n, at_pair(i), :] = v.astype(BF16)
                    acc[pl.ds(kept(h, m) + i * 2, 2)] = v.reshape(2, HSUB, 128)

                unrolled(half // 2, whole)

                @pl.when(m < n_blk - 1)
                def _():
                    window(1, m + 1).start()

                @pl.when(m < 4)
                def _():
                    link(h, m).start()

            return carry

        lax.fori_loop(0, n_blk + 1, body, 0)

    def combine_relay(h):
        relay_part(h, 4, 1, kept(h, 4))
        relay_part(h, 5, 0, kept(h, 5))

    def final(h):
        for n in (2, 3, 4, 5):
            link(h, n).wait_recv()
        for lo, n1, n2 in ((0, 2, 5), (half, 3, 4)):
            def fn(i, lo=lo, n1=n1, n2=n2):
                v = acc[pl.ds(kept(h, 6) + i * 2 + lo, 2)].reshape(pr, 128)
                v = v + lrecv[h, n1, at_pair(i), :].astype(F32) + lrecv[h, n2, at_pair(i), :].astype(F32)
                for q in range(2):
                    t = (i * 2 + q) + lo
                    xr = jnp.concatenate([xall[h * (HSUB // CSUB) + m][me * tok + t] for m in range(HSUB // CSUB)], axis=0).astype(F32)
                    ybuf[t, h * HSUB:(h + 1) * HSUB, :] = (v[q * HSUB:(q + 1) * HSUB, :] + xr).astype(BF16)

            pairs(fn)

    acc[zero_row] = jnp.zeros((HSUB, 128), F32)

    def half_step(h, carry):
        window(0, 0).start()
        window(1, 0).start()
        down(h)

        @pl.when(h > 0)
        def _():
            combine_relay(h - 1)

        combine_send(h)
        return carry

    lax.fori_loop(0, nh, half_step, 0)
    combine_relay(nh - 1)
    for h in range(nh):
        final(h)
    out = pltpu.make_async_copy(ybuf.at[0:tok], y_hbm, ysem.at[0])
    out.start()
    for k in range(nc):
        for n in range(13):
            ag(k, n).wait_send()
    for h in range(nh):
        for b in range(n_blk):
            d2d(h, b).wait_send()
        for n in range(6):
            link(h, n).wait_send()
    out.wait()


def solution(mesh):
    ep_axes = tuple(mesh.axis_names)
    n_dev = math.prod(mesh.shape[a] for a in ep_axes)
    row_spec = P(ep_axes, None)
    w_spec = P(ep_axes, None, None)

    def local_layer(tokens, expert_ids, gate_weights, w_gate, w_up, w_down):
        tok, hidden = tokens.shape
        topk = expert_ids.shape[1]
        n_loc, _, ff = w_gate.shape
        per_exp = n_dev * tok * topk // (n_dev * n_loc)
        kc, hc = CSUB * 128, HSUB * 128
        nc, nh = hidden // kc, hidden // hc
        n_tok = n_dev * tok
        half = tok // 2
        acc_rows = max(2 * n_loc * per_exp * (ff // 128), (n_loc * per_exp + 8) * HSUB + nh * 8 * half * HSUB)
        dims = (tok, hidden, ff, n_loc, per_exp, topk)
        scratch = [
            [pltpu.VMEM((n_tok + 8, CSUB, 128), BF16) for _ in range(nc)],
            pltpu.VMEM((n_dev, topk, tok), jnp.int32),
            pltpu.VMEM((n_dev, topk, tok), F32),
            pltpu.VMEM((n_dev + 1, n_loc, tok), jnp.int32),
            pltpu.VMEM((n_dev + 1, n_loc, tok), F32),
            pltpu.VMEM((n_loc + 8, 256), jnp.int32),
            pltpu.VMEM((n_tok // 16, 128), jnp.int32),
            pltpu.VMEM((n_tok, 128), jnp.int32),
            pltpu.VMEM((8 * (per_exp + 8), 128), F32),
            pltpu.VMEM((per_exp, kc), BF16),
            pltpu.VMEM((acc_rows // 8, 8, 128), F32),
            pltpu.VMEM((n_loc, per_exp, ff), BF16),
            pltpu.VMEM((RING, max(3 * kc, ff), hc), BF16),
            pltpu.VMEM((nh, 8, half * HSUB, 128), BF16),
            pltpu.VMEM((nh, 8, half * HSUB, 128), BF16),
            pltpu.VMEM((nh, 6, half * HSUB, 128), BF16),
            pltpu.VMEM((nh, 6, half * HSUB, 128), BF16),
            pltpu.VMEM((tok + 1, hidden // 128, 128), BF16),
            pltpu.SMEM((n_loc, 256), jnp.int32),
            pltpu.SMEM((8, 128), jnp.int32),
            pltpu.SMEM((8, 128), jnp.int32),
            pltpu.VMEM((2, 8, 8, 128), jnp.int32),
            pltpu.SemaphoreType.DMA((nc,)),
            pltpu.SemaphoreType.DMA((4,)),
            pltpu.SemaphoreType.DMA((2, n_dev - 1)),
            pltpu.SemaphoreType.DMA((2, n_dev - 1)),
            pltpu.SemaphoreType.DMA((nc, 13)),
            pltpu.SemaphoreType.DMA((nc, 13)),
            pltpu.SemaphoreType.DMA((RING, 4)),
            pltpu.SemaphoreType.DMA((nh, 8)),
            pltpu.SemaphoreType.DMA((nh, 8)),
            pltpu.SemaphoreType.DMA((nh, 6)),
            pltpu.SemaphoreType.DMA((nh, 6)),
            pltpu.SemaphoreType.DMA((1,)),
            pltpu.SemaphoreType.DMA((2,)),
        ]
        out = pl.pallas_call(
            functools.partial(moe_kernel, dims),
            out_shape=jax.ShapeDtypeStruct((tok, hidden // 128, 128), BF16),
            in_specs=[pl.BlockSpec(memory_space=pl.ANY)] * 6,
            out_specs=pl.BlockSpec(memory_space=pl.ANY),
            scratch_shapes=scratch,
            compiler_params=pltpu.CompilerParams(collective_id=0, has_side_effects=True,
                                                 vmem_limit_bytes=67043328),
        )(tokens, expert_ids.T, gate_weights.T, w_gate, w_up, w_down)
        return out.reshape(tok, hidden)

    return jax.shard_map(local_layer, mesh=mesh, in_specs=(row_spec, row_spec, row_spec, w_spec, w_spec, w_spec), out_specs=row_spec, check_vma=False)
```

```python
import functools
import math

import jax
import jax.numpy as jnp
from jax import lax
from jax.experimental import pallas as pl
from jax.experimental.pallas import tpu as pltpu
from jax.sharding import PartitionSpec as P

MESH = pl.DeviceIdType.MESH
F32 = jnp.float32
BF16 = jnp.bfloat16
RING = 5
CSUB = 4
HSUB = 8
TBLK = 64
TGRP = 4
UNROLL = 8


def unrolled(n, fn):
    def body(i, carry):
        fn(jnp.minimum(i, n - 1))
        return carry
    lax.fori_loop(0, n + 1, body, 0, unroll=n)


def moe_kernel(dims, x_hbm, ids_hbm, gts_hbm, w1_hbm, w3_hbm, w2_hbm, y_hbm,
               xall, ids_all, gts_all, chosen_pos, gate_tab, tok_tab, row_tab, pos_col, xg, xb, acc, hid, ring,
               psend, drecv, qsend, lrecv, ybuf, tok_sm, win_p, win_m, row_ord,
               loc_sem, tab_sem, rsend, rrecv, asend, arecv, wsem, dsend, drsem, lsend, lrsem, ysem, row_sem):
    tok, hidden, ff, n_loc, per_exp, topk = dims
    nc = hidden // (CSUB * 128)
    kc = CSUB * 128
    nh = hidden // (HSUB * 128)
    hc = HSUB * 128
    half = tok // 2
    n_dev = 8
    ct_ff = ff // 128
    zero_row = n_loc * per_exp
    xs = per_exp + 8

    z, y, c = lax.axis_index("ez"), lax.axis_index("ey"), lax.axis_index("ex")
    me = z * 4 + y * 2 + c
    xn, yn, pn = (z, 1 - y, c), (1 - z, y, c), (z, y, 1 - c)
    i_x = z * 4 + (1 - y) * 2 + c
    i_y = (1 - z) * 4 + y * 2 + c
    i_d = (1 - z) * 4 + (1 - y) * 2 + c

    def flip(i):
        b2, b1, b0 = (i >> 2) & 1, (i >> 1) & 1, i & 1
        t = (1 - z if b2 else z, 1 - y if b1 else y, 1 - c if b0 else c)
        return t, t[0] * 4 + t[1] * 2 + t[2]

    tail = ff - hc

    def w13_copies(k, e, slot):
        out = []
        for m, w in enumerate((w1_hbm, w3_hbm)):
            rows = pl.ds(k * kc, kc)
            out.append(pltpu.make_async_copy(w.at[e, rows, pl.ds(0, hc)], ring.at[slot, pl.ds(m * kc, kc), pl.ds(0, hc)], wsem.at[slot, 2 * m]))
            out.append(pltpu.make_async_copy(w.at[e, rows, pl.ds(hc, tail)], ring.at[slot, pl.ds(2 * kc, kc), pl.ds(m * tail, tail)],
                                             wsem.at[slot, 2 * m + 1]))
        return out

    def w2_copy(h, e, slot):
        return pltpu.make_async_copy(w2_hbm.at[e, :, pl.ds(pl.multiple_of(h * hc, hc), hc)], ring.at[slot, pl.ds(0, ff)],
                                     wsem.at[slot, 0])

    def weight(slot, m, ct, w):
        if ct * 128 < hc:
            return ring[slot, m * kc:(m + 1) * kc, ct * 128:(ct + w) * 128]
        c0 = m * tail + ct * 128 - hc
        return ring[slot, 2 * kc:3 * kc, c0:c0 + w * 128]

    own = pl.ds(pl.multiple_of(me * tok, tok), tok)
    loc = [pltpu.make_async_copy(x_hbm.at[pl.ds(0, tok), pl.ds(k * hc, hc)], ring.at[RING - 1, pl.ds(k * tok, tok)], loc_sem.at[k])
           for k in range(nh)]
    rlocs = [pltpu.make_async_copy(ids_hbm, ids_all.at[me], tab_sem.at[0]),
             pltpu.make_async_copy(gts_hbm, gts_all.at[me], tab_sem.at[3])]
    for cp in rlocs:
        cp.start()
    for cp in loc:
        cp.start()
    barrier = pltpu.get_barrier_semaphore()
    for i in range(1, n_dev):
        pl.semaphore_signal(barrier, inc=1, device_id=flip(i)[0], device_id_type=MESH)
    for e in range(RING - 1):
        for cp in w13_copies(0, e, e):
            cp.start()

    def own_rows(k):
        at = k * CSUB // HSUB
        for ct in range(CSUB):
            col = (k * CSUB + ct) % HSUB * 128
            xg[pl.ds(ct, tok, stride=CSUB), :] = ring[RING - 1, at * tok:(at + 1) * tok, col:col + 128].astype(F32)

        def one(t):
            xall[k][me * tok + t] = xg[pl.ds(pl.multiple_of(t * CSUB, CSUB), CSUB), :].astype(BF16)

        unrolled(tok, one)

    loc[0].wait()
    own_rows(0)
    pl.semaphore_wait(barrier, n_dev - 1)

    for cp in rlocs:
        cp.wait()
    rcopies = []
    for i in range(1, n_dev):
        for q, ref in enumerate((ids_all, gts_all)):
            cp = pltpu.make_async_remote_copy(ref.at[me], ref.at[me], rsend.at[q, i - 1], rrecv.at[q, i - 1],
                                              device_id=flip(i)[0], device_id_type=MESH)
            cp.start()
            rcopies.append(cp)

    def region(k, dev, lo, n):
        return xall[k].at[pl.ds(pl.multiple_of(dev * tok + lo, half), n)]

    partner_of = lambda d: d + 1 - 2 * c
    i_p = partner_of(me)
    flows = [
        (xn, me, i_x, 0, half), (xn, me, i_x, half, half), (xn, i_y, i_d, half, half),
        (yn, me, i_y, half, half), (yn, me, i_y, 0, half), (yn, i_x, i_d, 0, half),
        (pn, me, i_p, 0, tok),
        (pn, i_x, partner_of(i_x), 0, half), (pn, i_x, partner_of(i_x), half, half),
        (pn, i_y, partner_of(i_y), half, half), (pn, i_y, partner_of(i_y), 0, half),
        (pn, i_d, partner_of(i_d), 0, half), (pn, i_d, partner_of(i_d), half, half),
    ]

    def ag(k, n):
        tgt, src, _, lo, rows = flows[n]
        return pltpu.make_async_remote_copy(region(k, src, lo, rows), region(k, src, lo, rows),
                                            asend.at[k, n], arecv.at[k, n], device_id=tgt, device_id_type=MESH)

    def ag_recv(k, n):
        tgt, _, src, lo, rows = flows[n]
        pltpu.make_async_remote_copy(region(k, src, lo, rows), region(k, src, lo, rows),
                                     asend.at[k, n], arecv.at[k, n], device_id=tgt, device_id_type=MESH).wait_recv()

    def own_sends(k):
        for n in (0, 3, 1, 4, 6):
            ag(k, n).start()

    def relay1(k):
        ag_recv(k, 0)
        ag(k, 5).start()
        ag(k, 7).start()
        ag_recv(k, 3)
        ag(k, 2).start()
        ag(k, 9).start()

    def relay2(k):
        ag_recv(k, 1)
        ag(k, 8).start()
        ag_recv(k, 4)
        ag(k, 10).start()

    def relay3(k):
        ag_recv(k, 5)
        ag(k, 11).start()
        ag_recv(k, 2)
        ag(k, 12).start()

    def finish(k):
        for n in (6, 7, 9, 8, 10, 11, 12):
            ag_recv(k, n)

    own_sends(0)
    for k in range(1, nc):
        if k * CSUB % HSUB == 0:
            loc[k * CSUB // HSUB].wait()
        own_rows(k)
    for cp in w13_copies(0, RING - 1, RING - 1):
        cp.start()

    for cp in rcopies:
        cp.wait()
    base = me * n_loc
    my_ids = lax.broadcasted_iota(jnp.int32, (n_loc, tok), 0) + base
    off = jnp.zeros((n_loc, 1), jnp.int32)
    for s in range(n_dev):
        ids_s = ids_all[s]
        gts_s = gts_all[s]
        hit = jnp.zeros((n_loc, tok), jnp.int32)
        gden = jnp.zeros((n_loc, tok), F32)
        for j in range(topk):
            m = ids_s[j:j + 1, :] == my_ids
            hit = jnp.where(m, 1, hit)
            gden = gden + jnp.where(m, gts_s[j:j + 1, :], 0.0)
        cum = hit
        step = 1
        while step < tok:
            cum = cum + jnp.concatenate([jnp.zeros((n_loc, step), jnp.int32), cum[:, 0:tok - step]], axis=1)
            step *= 2
        pos = off + cum - 1
        off = off + cum[:, tok - 1:tok]
        posm = jnp.where(hit > 0, pos, -1)
        chosen_pos[s] = posm
        pos_col[s * tok:(s + 1) * tok, 0:n_loc] = posm.T
        gate_tab[s] = gden
        rows = jnp.full((topk, tok), zero_row, jnp.int32)
        for e in range(n_loc):
            rows = jnp.where(ids_s == base + e, e * per_exp + pos[e:e + 1, :], rows)
        for q in range(tok // 128):
            at = (s * (tok // 128) + q) * 8
            row_tab[at:at + topk, :] = rows[:, q * 128:(q + 1) * 128] * HSUB
            row_tab[at + topk:at + 8, :] = jnp.zeros((8 - topk, 128), jnp.int32)
    order = [(i_d, 0), (i_d, 1), (i_x, 0), (i_y, 1), (i_x, 1), (i_y, 0), (me, 0), (me, 1)]
    n_blk = len(order)
    for b, (dev, hf) in enumerate(order):
        for side, d in enumerate((partner_of(dev), dev)):
            row_ord[side, b] = row_tab[pl.ds(pl.multiple_of((d * 2 + hf) * 8, 8), 8), :]

    def window(side, b):
        return pltpu.make_async_copy(row_ord.at[side, b], (win_p, win_m)[side], row_sem.at[side])

    relay1(0)
    own_sends(1)
    relay2(0)
    lpos = lax.broadcasted_iota(jnp.int32, (TBLK, per_exp), 1)
    tcol = lax.broadcasted_iota(jnp.int32, (TBLK, per_exp), 0)
    for e0 in range(0, n_loc, TGRP):
        def tok_step(i, sums, e0=e0):
            pc = pos_col[pl.ds(pl.multiple_of(i * TBLK, TBLK), TBLK), :]
            out = []
            for e in range(TGRP):
                hitv = jnp.where(pc[:, e0 + e:e0 + e + 1] == lpos, tcol + i * TBLK, 0)
                out.append(sums[e] + jnp.sum(hitv.reshape(TBLK // 8, 8, per_exp), axis=0))
            return tuple(out)

        sums = lax.fori_loop(0, n_dev * tok // TBLK, tok_step,
                             tuple(jnp.zeros((8, per_exp), jnp.int32) for _ in range(TGRP)), unroll=4)
        for e in range(TGRP):
            tok_tab[e0 + e:e0 + e + 1, 0:per_exp] = jnp.sum(sums[e], axis=0, keepdims=True)

    tok_cp = pltpu.make_async_copy(tok_tab.at[0:n_loc], tok_sm, tab_sem.at[2])
    tok_cp.start()

    relay3(0)

    tok_cp.wait()
    finish(0)
    relay1(1)
    own_sends(2)

    def acc_row(e, mat, ct):
        return ((e * 2 + mat) * ct_ff + ct) * (per_exp // 8)

    def pick(k, e, lo, n):
        def one(i):
            xg[pl.ds(lo + i, CSUB, stride=xs), :] = xall[k][tok_sm[e, lo + i]].astype(F32)

        unrolled(n, one)

    def proj_step(k, e):
        slot = lax.rem(k * n_loc + e, RING)
        for cp in w13_copies(k, e, slot):
            cp.wait()
        for ct in range(CSUB):
            xb[:, ct * 128:(ct + 1) * 128] = xg[ct * xs:ct * xs + per_exp, :].astype(BF16)
        nxt = jnp.minimum(e + 1, n_loc - 1)
        steps = list(range(0, ct_ff, 2))
        share = per_exp // len(steps)
        for si, ct in enumerate(steps):
            w = min(2, ct_ff - ct)
            if w == 2:
                d = [jnp.dot(xb[...], weight(slot, mat, ct, w), preferred_element_type=F32) for mat in range(2)]
            else:
                both = jnp.concatenate([weight(slot, mat, ct, w) for mat in range(2)], axis=1)
                r = jnp.dot(xb[...], both, preferred_element_type=F32)
                d = [r[:, 0:128], r[:, 128:256]]
            pick(k, nxt, si * share, share)
            for q in range(w):
                parts = []
                for mat in range(2):
                    at = pl.ds(acc_row(e, mat, ct + q), per_exp // 8)
                    v = d[mat][:, q * 128:(q + 1) * 128]
                    if k > 0:
                        v = v + acc[at].reshape(per_exp, 128)
                    if k < nc - 1:
                        acc[at] = v.reshape(per_exp // 8, 8, 128)
                    parts.append(v)
                if k == nc - 1:
                    hid[e, :, (ct + q) * 128:(ct + q + 1) * 128] = (jax.nn.silu(parts[0]) * parts[1]).astype(BF16)
        @pl.when(e < n_loc - RING)
        def _():
            for cp in w13_copies(k, e + RING, slot):
                cp.start()

        @pl.when(e >= n_loc - RING)
        def _():
            if k < nc - 1:
                for cp in w13_copies(k + 1, e + RING - n_loc, slot):
                    cp.start()
            else:
                w2_copy(0, e + RING - n_loc, slot).start()

    for k in range(nc):
        pick(k, 0, 0, per_exp)

        def body(e, carry, k=k):
            proj_step(k, e)
            if k + 1 < nc:
                if k > 0:
                    @pl.when(e == 1)
                    def _():
                        relay1(k + 1)
                        if k + 2 < nc:
                            own_sends(k + 2)

                @pl.when(e == (4 if k > 0 else 1))
                def _():
                    relay2(k + 1)

                @pl.when(e == 6)
                def _():
                    relay3(k + 1)
            return carry

        lax.fori_loop(0, n_loc, body, 0)
        if k + 1 < nc:
            finish(k + 1)

    flat = acc.reshape(acc.shape[0] * 8, 128)

    def down(h):
        def body(e, carry):
            step = h * n_loc + e
            slot = lax.rem(nc * n_loc + step, RING)
            w2_copy(h, e, slot).wait()
            ipos = lax.broadcasted_iota(jnp.int32, (per_exp, tok), 0)
            gsum = jnp.zeros((per_exp, tok), F32)
            for s in range(n_dev):
                prow = chosen_pos[s, pl.ds(e, 1), :]
                grow = gate_tab[s, pl.ds(e, 1), :]
                gsum = gsum + jnp.where(prow == ipos, grow, 0.0)
            g = jnp.broadcast_to(jnp.sum(gsum, axis=1, keepdims=True), (per_exp, 128))
            for n in range(0, HSUB, 2):
                o = jnp.dot(hid[e], ring[slot, 0:ff, n * 128:(n + 2) * 128], preferred_element_type=F32)
                for q in range(2):
                    flat[pl.ds(e * (per_exp * HSUB) + n + q, per_exp, stride=HSUB), :] = o[:, q * 128:(q + 1) * 128] * g

            @pl.when(e < n_loc - RING)
            def _():
                w2_copy(h, e + RING, slot).start()

            @pl.when(jnp.logical_and(e >= n_loc - RING, h < nh - 1))
            def _():
                w2_copy(h + 1, e + RING - n_loc, slot).start()

            return carry

        lax.fori_loop(0, n_loc, body, 0)

    def pair_sum(win, i):
        out = []
        for t in (2 * i, 2 * i + 1):
            v = flat[pl.ds(win[0, t], HSUB), :]
            for j in range(1, topk):
                v = v + flat[pl.ds(win[j, t], HSUB), :]
            out.append(v)
        return jnp.concatenate(out, axis=0)

    pr = 2 * HSUB
    f_base = zero_row + 8

    def at_pair(i):
        return pl.ds(i * pr if isinstance(i, int) else pl.multiple_of(i * pr, pr), pr)

    def kept(h, b):
        return f_base + (h * n_blk + b) * half

    def d2d(h, b):
        return pltpu.make_async_remote_copy(psend.at[h, b], drecv.at[h, b], dsend.at[h, b], drsem.at[h, b],
                                            device_id=pn, device_id_type=MESH)

    def link(h, n):
        par = n % 2 if isinstance(n, int) else lax.rem(n, 2)
        tgt = (z + par * (1 - 2 * z), y + (1 - par) * (1 - 2 * y), c)
        return pltpu.make_async_remote_copy(qsend.at[h, n], lrecv.at[h, n], lsend.at[h, n], lrsem.at[h, n],
                                            device_id=tgt, device_id_type=MESH)

    def pairs(fn):
        def body(i, carry):
            for u in range(UNROLL):
                fn(i * UNROLL + u)
            return carry
        lax.fori_loop(0, half // (2 * UNROLL), body, 0)

    def relay_part(h, n, rn, base):
        link(h, rn).wait_recv()

        def fn(i):
            v = acc[pl.ds(base + i * 2, 2)].reshape(pr, 128)
            qsend[h, n, at_pair(i), :] = (v + lrecv[h, rn, at_pair(i), :].astype(F32)).astype(BF16)

        pairs(fn)
        link(h, n).start()

    def combine_relay(h):
        relay_part(h, 4, 1, kept(h, 4))
        relay_part(h, 5, 0, kept(h, 5))

    def combine_send(h):
        def body(b, carry):
            @pl.when(b < n_blk)
            def _():
                window(0, b).wait()

                def part(i):
                    psend[h, b, at_pair(i), :] = pair_sum(win_p, i).astype(BF16)

                unrolled(half // 2, part)
                d2d(h, b).start()

                @pl.when(b < n_blk - 1)
                def _():
                    window(0, b + 1).start()

            @pl.when(b > 0)
            def _():
                m = b - 1
                d2d(h, m).wait_recv()
                window(1, m).wait()
                n = jnp.minimum(m, 6)

                def whole(i):
                    v = pair_sum(win_m, i) + drecv[h, m, at_pair(i), :].astype(F32)
                    qsend[h, n, at_pair(i), :] = v.astype(BF16)
                    acc[pl.ds(kept(h, m) + i * 2, 2)] = v.reshape(2, HSUB, 128)

                unrolled(half // 2, whole)

                @pl.when(m < n_blk - 1)
                def _():
                    window(1, m + 1).start()

                @pl.when(m < 4)
                def _():
                    link(h, m).start()

                @pl.when(m == n_blk - 1)
                def _():
                    combine_relay(h)

            return carry

        lax.fori_loop(0, n_blk + 1, body, 0)

    def final(h):
        for n in (2, 3, 4, 5):
            link(h, n).wait_recv()
        for lo, n1, n2 in ((0, 2, 5), (half, 3, 4)):
            def fn(i, lo=lo, n1=n1, n2=n2):
                v = acc[pl.ds(kept(h, 6) + i * 2 + lo, 2)].reshape(pr, 128)
                v = v + lrecv[h, n1, at_pair(i), :].astype(F32) + lrecv[h, n2, at_pair(i), :].astype(F32)
                for q in range(2):
                    t = (i * 2 + q) + lo
                    xr = jnp.concatenate([xall[h * (HSUB // CSUB) + m][me * tok + t] for m in range(HSUB // CSUB)], axis=0).astype(F32)
                    ybuf[t, h * HSUB:(h + 1) * HSUB, :] = (v[q * HSUB:(q + 1) * HSUB, :] + xr).astype(BF16)

            pairs(fn)

    acc[zero_row] = jnp.zeros((HSUB, 128), F32)

    def half_step(h, carry):
        window(0, 0).start()
        window(1, 0).start()
        down(h)

        combine_send(h)
        return carry

    lax.fori_loop(0, nh, half_step, 0)
    outs = []
    for h in range(nh):
        final(h)
        out = pltpu.make_async_copy(ybuf.at[pl.ds(0, tok), pl.ds(h * HSUB, HSUB)], y_hbm.at[pl.ds(0, tok), pl.ds(h * HSUB, HSUB)],
                                    ysem.at[h])
        out.start()
        outs.append(out)
    for k in range(nc):
        for n in range(13):
            ag(k, n).wait_send()
    for h in range(nh):
        for b in range(n_blk):
            d2d(h, b).wait_send()
        for n in range(6):
            link(h, n).wait_send()
    for out in outs:
        out.wait()


def solution(mesh):
    ep_axes = tuple(mesh.axis_names)
    n_dev = math.prod(mesh.shape[a] for a in ep_axes)
    row_spec = P(ep_axes, None)
    w_spec = P(ep_axes, None, None)

    def local_layer(tokens, expert_ids, gate_weights, w_gate, w_up, w_down):
        tok, hidden = tokens.shape
        topk = expert_ids.shape[1]
        n_loc, _, ff = w_gate.shape
        per_exp = n_dev * tok * topk // (n_dev * n_loc)
        kc, hc = CSUB * 128, HSUB * 128
        nc, nh = hidden // kc, hidden // hc
        n_tok = n_dev * tok
        half = tok // 2
        acc_rows = max(2 * n_loc * per_exp * (ff // 128), (n_loc * per_exp + 8) * HSUB + nh * 8 * half * HSUB)
        dims = (tok, hidden, ff, n_loc, per_exp, topk)
        scratch = [
            [pltpu.VMEM((n_tok + 8, CSUB, 128), BF16) for _ in range(nc)],
            pltpu.VMEM((n_dev, topk, tok), jnp.int32),
            pltpu.VMEM((n_dev, topk, tok), F32),
            pltpu.VMEM((n_dev + 1, n_loc, tok), jnp.int32),
            pltpu.VMEM((n_dev + 1, n_loc, tok), F32),
            pltpu.VMEM((n_loc + 8, 256), jnp.int32),
            pltpu.VMEM((n_tok // 16, 128), jnp.int32),
            pltpu.VMEM((n_tok, 128), jnp.int32),
            pltpu.VMEM((8 * (per_exp + 8), 128), F32),
            pltpu.VMEM((per_exp, kc), BF16),
            pltpu.VMEM((acc_rows // 8, 8, 128), F32),
            pltpu.VMEM((n_loc, per_exp, ff), BF16),
            pltpu.VMEM((RING, max(3 * kc, ff), hc), BF16),
            pltpu.VMEM((nh, 8, half * HSUB, 128), BF16),
            pltpu.VMEM((nh, 8, half * HSUB, 128), BF16),
            pltpu.VMEM((nh, 7, half * HSUB, 128), BF16),
            pltpu.VMEM((nh, 6, half * HSUB, 128), BF16),
            pltpu.VMEM((tok + 1, hidden // 128, 128), BF16),
            pltpu.SMEM((n_loc, 256), jnp.int32),
            pltpu.SMEM((8, 128), jnp.int32),
            pltpu.SMEM((8, 128), jnp.int32),
            pltpu.VMEM((2, 8, 8, 128), jnp.int32),
            pltpu.SemaphoreType.DMA((nc,)),
            pltpu.SemaphoreType.DMA((4,)),
            pltpu.SemaphoreType.DMA((2, n_dev - 1)),
            pltpu.SemaphoreType.DMA((2, n_dev - 1)),
            pltpu.SemaphoreType.DMA((nc, 13)),
            pltpu.SemaphoreType.DMA((nc, 13)),
            pltpu.SemaphoreType.DMA((RING, 4)),
            pltpu.SemaphoreType.DMA((nh, 8)),
            pltpu.SemaphoreType.DMA((nh, 8)),
            pltpu.SemaphoreType.DMA((nh, 6)),
            pltpu.SemaphoreType.DMA((nh, 6)),
            pltpu.SemaphoreType.DMA((nh,)),
            pltpu.SemaphoreType.DMA((2,)),
        ]
        out = pl.pallas_call(
            functools.partial(moe_kernel, dims),
            out_shape=jax.ShapeDtypeStruct((tok, hidden // 128, 128), BF16),
            in_specs=[pl.BlockSpec(memory_space=pl.ANY)] * 6,
            out_specs=pl.BlockSpec(memory_space=pl.ANY),
            scratch_shapes=scratch,
            compiler_params=pltpu.CompilerParams(collective_id=0, has_side_effects=True,
                                                 vmem_limit_bytes=67043328),
        )(tokens, expert_ids.T, gate_weights.T, w_gate, w_up, w_down)
        return out.reshape(tok, hidden)

    return jax.shard_map(local_layer, mesh=mesh, in_specs=(row_spec, row_spec, row_spec, w_spec, w_spec, w_spec), out_specs=row_spec, check_vma=False)
```

```python
import functools
import math

import jax
import jax.numpy as jnp
from jax import lax
from jax.experimental import pallas as pl
from jax.experimental.pallas import tpu as pltpu
from jax.sharding import PartitionSpec as P

MESH = pl.DeviceIdType.MESH
F32 = jnp.float32
BF16 = jnp.bfloat16
RING = 5
CSUB = 4
HSUB = 8
TBLK = 64
TGRP = 4
UNROLL = 8


def unrolled(n, fn):
    def body(i, carry):
        fn(jnp.minimum(i, n - 1))
        return carry
    lax.fori_loop(0, n + 1, body, 0, unroll=n)


def moe_kernel(dims, x_hbm, ids_hbm, gts_hbm, w1_hbm, w3_hbm, w2_hbm, y_hbm,
               xall, ids_all, gts_all, chosen_pos, gate_tab, tok_tab, row_tab, pos_col, gcol, xg, xb, acc, hid, ring,
               psend, drecv, qsend, lrecv, ybuf, tok_sm, win_p, win_m, row_ord,
               loc_sem, tab_sem, rsend, rrecv, asend, arecv, wsem, dsend, drsem, lsend, lrsem, ysem, row_sem):
    tok, hidden, ff, n_loc, per_exp, topk = dims
    nc = hidden // (CSUB * 128)
    kc = CSUB * 128
    nh = hidden // (HSUB * 128)
    hc = HSUB * 128
    half = tok // 2
    n_dev = 8
    ct_ff = ff // 128
    zero_row = n_loc * per_exp
    xs = per_exp + 8

    z, y, c = lax.axis_index("ez"), lax.axis_index("ey"), lax.axis_index("ex")
    me = z * 4 + y * 2 + c
    xn, yn, pn = (z, 1 - y, c), (1 - z, y, c), (z, y, 1 - c)
    i_x = z * 4 + (1 - y) * 2 + c
    i_y = (1 - z) * 4 + y * 2 + c
    i_d = (1 - z) * 4 + (1 - y) * 2 + c

    def flip(i):
        b2, b1, b0 = (i >> 2) & 1, (i >> 1) & 1, i & 1
        t = (1 - z if b2 else z, 1 - y if b1 else y, 1 - c if b0 else c)
        return t, t[0] * 4 + t[1] * 2 + t[2]

    tail = ff - hc

    def w13_copies(k, e, slot):
        out = []
        for m, w in enumerate((w1_hbm, w3_hbm)):
            rows = pl.ds(k * kc, kc)
            out.append(pltpu.make_async_copy(w.at[e, rows, pl.ds(0, hc)], ring.at[slot, pl.ds(m * kc, kc), pl.ds(0, hc)], wsem.at[slot, 2 * m]))
            out.append(pltpu.make_async_copy(w.at[e, rows, pl.ds(hc, tail)], ring.at[slot, pl.ds(2 * kc, kc), pl.ds(m * tail, tail)],
                                             wsem.at[slot, 2 * m + 1]))
        return out

    def w2_copy(h, e, slot):
        return pltpu.make_async_copy(w2_hbm.at[e, :, pl.ds(pl.multiple_of(h * hc, hc), hc)], ring.at[slot, pl.ds(0, ff)],
                                     wsem.at[slot, 0])

    def weight(slot, m, ct, w):
        if ct * 128 < hc:
            return ring[slot, m * kc:(m + 1) * kc, ct * 128:(ct + w) * 128]
        c0 = m * tail + ct * 128 - hc
        return ring[slot, 2 * kc:3 * kc, c0:c0 + w * 128]

    own = pl.ds(pl.multiple_of(me * tok, tok), tok)
    loc = [pltpu.make_async_copy(x_hbm.at[pl.ds(0, tok), pl.ds(k * hc, hc)], ring.at[RING - 1, pl.ds(k * tok, tok)], loc_sem.at[k])
           for k in range(nh)]
    rlocs = [pltpu.make_async_copy(ids_hbm, ids_all.at[me], tab_sem.at[0]),
             pltpu.make_async_copy(gts_hbm, gts_all.at[me], tab_sem.at[3])]
    for cp in rlocs:
        cp.start()
    for cp in loc:
        cp.start()
    barrier = pltpu.get_barrier_semaphore()
    for i in range(1, n_dev):
        pl.semaphore_signal(barrier, inc=1, device_id=flip(i)[0], device_id_type=MESH)
    for e in range(RING - 1):
        for cp in w13_copies(0, e, e):
            cp.start()

    def own_rows(k):
        at = k * CSUB // HSUB
        for ct in range(CSUB):
            col = (k * CSUB + ct) % HSUB * 128
            xg[pl.ds(ct, tok, stride=CSUB), :] = ring[RING - 1, at * tok:(at + 1) * tok, col:col + 128].astype(F32)

        def one(t):
            xall[k][me * tok + t] = xg[pl.ds(pl.multiple_of(t * CSUB, CSUB), CSUB), :].astype(BF16)

        unrolled(tok, one)

    loc[0].wait()
    own_rows(0)
    pl.semaphore_wait(barrier, n_dev - 1)

    for cp in rlocs:
        cp.wait()
    rcopies = []
    for i in range(1, n_dev):
        for q, ref in enumerate((ids_all, gts_all)):
            cp = pltpu.make_async_remote_copy(ref.at[me], ref.at[me], rsend.at[q, i - 1], rrecv.at[q, i - 1],
                                              device_id=flip(i)[0], device_id_type=MESH)
            cp.start()
            rcopies.append(cp)

    def region(k, dev, lo, n):
        return xall[k].at[pl.ds(pl.multiple_of(dev * tok + lo, half), n)]

    partner_of = lambda d: d + 1 - 2 * c
    i_p = partner_of(me)
    flows = [
        (xn, me, i_x, 0, half), (xn, me, i_x, half, half), (xn, i_y, i_d, half, half),
        (yn, me, i_y, half, half), (yn, me, i_y, 0, half), (yn, i_x, i_d, 0, half),
        (pn, me, i_p, 0, tok),
        (pn, i_x, partner_of(i_x), 0, half), (pn, i_x, partner_of(i_x), half, half),
        (pn, i_y, partner_of(i_y), half, half), (pn, i_y, partner_of(i_y), 0, half),
        (pn, i_d, partner_of(i_d), 0, half), (pn, i_d, partner_of(i_d), half, half),
    ]

    def ag(k, n):
        tgt, src, _, lo, rows = flows[n]
        return pltpu.make_async_remote_copy(region(k, src, lo, rows), region(k, src, lo, rows),
                                            asend.at[k, n], arecv.at[k, n], device_id=tgt, device_id_type=MESH)

    def ag_recv(k, n):
        tgt, _, src, lo, rows = flows[n]
        pltpu.make_async_remote_copy(region(k, src, lo, rows), region(k, src, lo, rows),
                                     asend.at[k, n], arecv.at[k, n], device_id=tgt, device_id_type=MESH).wait_recv()

    def own_sends(k):
        for n in (0, 3, 1, 4, 6):
            ag(k, n).start()

    def relay1(k):
        ag_recv(k, 0)
        ag(k, 5).start()
        ag(k, 7).start()
        ag_recv(k, 3)
        ag(k, 2).start()
        ag(k, 9).start()

    def relay2(k):
        ag_recv(k, 1)
        ag(k, 8).start()
        ag_recv(k, 4)
        ag(k, 10).start()

    def relay3(k):
        ag_recv(k, 5)
        ag(k, 11).start()
        ag_recv(k, 2)
        ag(k, 12).start()

    def finish(k):
        for n in (6, 7, 9, 8, 10, 11, 12):
            ag_recv(k, n)

    own_sends(0)
    for k in range(1, nc):
        if k * CSUB % HSUB == 0:
            loc[k * CSUB // HSUB].wait()
        own_rows(k)
    for cp in w13_copies(0, RING - 1, RING - 1):
        cp.start()

    for cp in rcopies:
        cp.wait()
    base = me * n_loc
    my_ids = lax.broadcasted_iota(jnp.int32, (n_loc, tok), 0) + base
    off = jnp.zeros((n_loc, 1), jnp.int32)
    for s in range(n_dev):
        ids_s = ids_all[s]
        gts_s = gts_all[s]
        hit = jnp.zeros((n_loc, tok), jnp.int32)
        gden = jnp.zeros((n_loc, tok), F32)
        for j in range(topk):
            m = ids_s[j:j + 1, :] == my_ids
            hit = jnp.where(m, 1, hit)
            gden = gden + jnp.where(m, gts_s[j:j + 1, :], 0.0)
        cum = hit
        step = 1
        while step < tok:
            cum = cum + jnp.concatenate([jnp.zeros((n_loc, step), jnp.int32), cum[:, 0:tok - step]], axis=1)
            step *= 2
        pos = off + cum - 1
        off = off + cum[:, tok - 1:tok]
        posm = jnp.where(hit > 0, pos, -1)
        chosen_pos[s] = posm
        pos_col[s * tok:(s + 1) * tok, 0:n_loc] = posm.T
        gate_tab[s] = gden
        rows = jnp.full((topk, tok), zero_row, jnp.int32)
        for e in range(n_loc):
            rows = jnp.where(ids_s == base + e, e * per_exp + pos[e:e + 1, :], rows)
        for q in range(tok // 128):
            at = (s * (tok // 128) + q) * 8
            row_tab[at:at + topk, :] = rows[:, q * 128:(q + 1) * 128] * HSUB
            row_tab[at + topk:at + 8, :] = jnp.zeros((8 - topk, 128), jnp.int32)
    order = [(i_d, 0), (i_d, 1), (i_x, 0), (i_y, 1), (i_x, 1), (i_y, 0), (me, 0), (me, 1)]
    n_blk = len(order)
    for b, (dev, hf) in enumerate(order):
        for side, d in enumerate((partner_of(dev), dev)):
            row_ord[side, b] = row_tab[pl.ds(pl.multiple_of((d * 2 + hf) * 8, 8), 8), :]

    def window(side, b):
        return pltpu.make_async_copy(row_ord.at[side, b], (win_p, win_m)[side], row_sem.at[side])

    relay1(0)
    own_sends(1)
    relay2(0)
    lpos = lax.broadcasted_iota(jnp.int32, (TBLK, per_exp), 1)
    tcol = lax.broadcasted_iota(jnp.int32, (TBLK, per_exp), 0)
    for e0 in range(0, n_loc, TGRP):
        def tok_step(i, sums, e0=e0):
            pc = pos_col[pl.ds(pl.multiple_of(i * TBLK, TBLK), TBLK), :]
            out = []
            for e in range(TGRP):
                hitv = jnp.where(pc[:, e0 + e:e0 + e + 1] == lpos, tcol + i * TBLK, 0)
                out.append(sums[e] + jnp.sum(hitv.reshape(TBLK // 8, 8, per_exp), axis=0))
            return tuple(out)

        sums = lax.fori_loop(0, n_dev * tok // TBLK, tok_step,
                             tuple(jnp.zeros((8, per_exp), jnp.int32) for _ in range(TGRP)), unroll=4)
        for e in range(TGRP):
            tok_tab[e0 + e:e0 + e + 1, 0:per_exp] = jnp.sum(sums[e], axis=0, keepdims=True)

    tok_cp = pltpu.make_async_copy(tok_tab.at[0:n_loc], tok_sm, tab_sem.at[2])
    tok_cp.start()

    relay3(0)

    tok_cp.wait()
    finish(0)
    relay1(1)
    own_sends(2)

    def acc_row(e, mat, ct):
        return ((e * 2 + mat) * ct_ff + ct) * (per_exp // 8)

    def pick(k, e, lo, n):
        def one(i):
            xg[pl.ds(lo + i, CSUB, stride=xs), :] = xall[k][tok_sm[e, lo + i]].astype(F32)

        unrolled(n, one)

    def gate_column(e):
        ipos = lax.broadcasted_iota(jnp.int32, (per_exp, tok), 0)
        gsum = jnp.zeros((per_exp, tok), F32)
        for s in range(n_dev):
            prow = chosen_pos[s, pl.ds(e, 1), :]
            grow = gate_tab[s, pl.ds(e, 1), :]
            gsum = gsum + jnp.where(prow == ipos, grow, 0.0)
        gcol[e] = jnp.broadcast_to(jnp.sum(gsum, axis=1, keepdims=True), (per_exp, 128))

    def proj_step(k, e):
        slot = lax.rem(k * n_loc + e, RING)
        for cp in w13_copies(k, e, slot):
            cp.wait()
        for ct in range(CSUB):
            xb[:, ct * 128:(ct + 1) * 128] = xg[ct * xs:ct * xs + per_exp, :].astype(BF16)
        nxt = jnp.minimum(e + 1, n_loc - 1)
        if k == 1:
            gate_column(e)
        steps = list(range(0, ct_ff, 2))
        share = per_exp // len(steps)
        for si, ct in enumerate(steps):
            w = min(2, ct_ff - ct)
            if w == 2:
                d = [jnp.dot(xb[...], weight(slot, mat, ct, w), preferred_element_type=F32) for mat in range(2)]
            else:
                both = jnp.concatenate([weight(slot, mat, ct, w) for mat in range(2)], axis=1)
                r = jnp.dot(xb[...], both, preferred_element_type=F32)
                d = [r[:, 0:128], r[:, 128:256]]
            pick(k, nxt, si * share, share)
            for q in range(w):
                parts = []
                for mat in range(2):
                    at = pl.ds(acc_row(e, mat, ct + q), per_exp // 8)
                    v = d[mat][:, q * 128:(q + 1) * 128]
                    if k > 0:
                        v = v + acc[at].reshape(per_exp, 128)
                    if k < nc - 1:
                        acc[at] = v.reshape(per_exp // 8, 8, 128)
                    parts.append(v)
                if k == nc - 1:
                    hid[e, :, (ct + q) * 128:(ct + q + 1) * 128] = (jax.nn.silu(parts[0]) * parts[1]).astype(BF16)
        @pl.when(e < n_loc - RING)
        def _():
            for cp in w13_copies(k, e + RING, slot):
                cp.start()

        @pl.when(e >= n_loc - RING)
        def _():
            if k < nc - 1:
                for cp in w13_copies(k + 1, e + RING - n_loc, slot):
                    cp.start()
            else:
                w2_copy(0, e + RING - n_loc, slot).start()

    for k in range(nc):
        pick(k, 0, 0, per_exp)

        def body(e, carry, k=k):
            proj_step(k, e)
            if k + 1 < nc:
                if k > 0:
                    @pl.when(e == 1)
                    def _():
                        relay1(k + 1)
                        if k + 2 < nc:
                            own_sends(k + 2)

                @pl.when(e == (4 if k > 0 else 1))
                def _():
                    relay2(k + 1)

                @pl.when(e == 6)
                def _():
                    relay3(k + 1)
            return carry

        lax.fori_loop(0, n_loc, body, 0)
        if k + 1 < nc:
            finish(k + 1)

    flat = acc.reshape(acc.shape[0] * 8, 128)

    def down(h):
        def body(e, carry):
            step = h * n_loc + e
            slot = lax.rem(nc * n_loc + step, RING)
            w2_copy(h, e, slot).wait()
            g = gcol[e]
            for n in range(0, HSUB, 2):
                o = jnp.dot(hid[e], ring[slot, 0:ff, n * 128:(n + 2) * 128], preferred_element_type=F32)
                for q in range(2):
                    flat[pl.ds(e * (per_exp * HSUB) + n + q, per_exp, stride=HSUB), :] = o[:, q * 128:(q + 1) * 128] * g

            @pl.when(e < n_loc - RING)
            def _():
                w2_copy(h, e + RING, slot).start()

            @pl.when(jnp.logical_and(e >= n_loc - RING, h < nh - 1))
            def _():
                w2_copy(h + 1, e + RING - n_loc, slot).start()

            return carry

        lax.fori_loop(0, n_loc, body, 0)

    def pair_sum(win, i):
        out = []
        for t in (2 * i, 2 * i + 1):
            v = flat[pl.ds(win[0, t], HSUB), :]
            for j in range(1, topk):
                v = v + flat[pl.ds(win[j, t], HSUB), :]
            out.append(v)
        return jnp.concatenate(out, axis=0)

    pr = 2 * HSUB
    f_base = zero_row + 8

    def at_pair(i):
        return pl.ds(i * pr if isinstance(i, int) else pl.multiple_of(i * pr, pr), pr)

    def kept(h, b):
        return f_base + (h * n_blk + b) * half

    def d2d(h, b):
        return pltpu.make_async_remote_copy(psend.at[h, b], drecv.at[h, b], dsend.at[h, b], drsem.at[h, b],
                                            device_id=pn, device_id_type=MESH)

    def link(h, n):
        par = n % 2 if isinstance(n, int) else lax.rem(n, 2)
        tgt = (z + par * (1 - 2 * z), y + (1 - par) * (1 - 2 * y), c)
        return pltpu.make_async_remote_copy(qsend.at[h, n], lrecv.at[h, n], lsend.at[h, n], lrsem.at[h, n],
                                            device_id=tgt, device_id_type=MESH)

    def pairs(fn):
        def body(i, carry):
            for u in range(UNROLL):
                fn(i * UNROLL + u)
            return carry
        lax.fori_loop(0, half // (2 * UNROLL), body, 0)

    def relay_part(h, n, rn, base):
        link(h, rn).wait_recv()

        def fn(i):
            v = acc[pl.ds(base + i * 2, 2)].reshape(pr, 128)
            qsend[h, n, at_pair(i), :] = (v + lrecv[h, rn, at_pair(i), :].astype(F32)).astype(BF16)

        pairs(fn)
        link(h, n).start()

    def combine_relay(h):
        relay_part(h, 4, 1, kept(h, 4))
        relay_part(h, 5, 0, kept(h, 5))

    def combine_send(h):
        def body(b, carry):
            @pl.when(b < n_blk)
            def _():
                window(0, b).wait()

                def part(i):
                    psend[h, b, at_pair(i), :] = pair_sum(win_p, i).astype(BF16)

                unrolled(half // 2, part)
                d2d(h, b).start()

                @pl.when(b < n_blk - 1)
                def _():
                    window(0, b + 1).start()

            @pl.when(b > 0)
            def _():
                m = b - 1
                d2d(h, m).wait_recv()
                window(1, m).wait()
                n = jnp.minimum(m, 6)

                def whole(i):
                    v = pair_sum(win_m, i) + drecv[h, m, at_pair(i), :].astype(F32)
                    qsend[h, n, at_pair(i), :] = v.astype(BF16)
                    acc[pl.ds(kept(h, m) + i * 2, 2)] = v.reshape(2, HSUB, 128)

                unrolled(half // 2, whole)

                @pl.when(m < n_blk - 1)
                def _():
                    window(1, m + 1).start()

                @pl.when(m < 4)
                def _():
                    link(h, m).start()

                @pl.when(m == n_blk - 1)
                def _():
                    combine_relay(h)

            return carry

        lax.fori_loop(0, n_blk + 1, body, 0)

    def final(h):
        for n in (2, 3, 4, 5):
            link(h, n).wait_recv()
        for lo, n1, n2 in ((0, 2, 5), (half, 3, 4)):
            def fn(i, lo=lo, n1=n1, n2=n2):
                v = acc[pl.ds(kept(h, 6) + i * 2 + lo, 2)].reshape(pr, 128)
                v = v + lrecv[h, n1, at_pair(i), :].astype(F32) + lrecv[h, n2, at_pair(i), :].astype(F32)
                for q in range(2):
                    t = (i * 2 + q) + lo
                    xr = jnp.concatenate([xall[h * (HSUB // CSUB) + m][me * tok + t] for m in range(HSUB // CSUB)], axis=0).astype(F32)
                    ybuf[t, h * HSUB:(h + 1) * HSUB, :] = (v[q * HSUB:(q + 1) * HSUB, :] + xr).astype(BF16)

            pairs(fn)

    acc[zero_row] = jnp.zeros((HSUB, 128), F32)

    def half_step(h, carry):
        window(0, 0).start()
        window(1, 0).start()
        down(h)

        combine_send(h)
        return carry

    lax.fori_loop(0, nh, half_step, 0)
    for k in range(nc):
        for n in range(13):
            ag(k, n).wait_send()
    for h in range(nh):
        for b in range(n_blk):
            d2d(h, b).wait_send()
        for n in range(6):
            if h < nh - 1 or n < 4:
                link(h, n).wait_send()
    outs = []
    for h in range(nh):
        final(h)
        out = pltpu.make_async_copy(ybuf.at[pl.ds(0, tok), pl.ds(h * HSUB, HSUB)], y_hbm.at[pl.ds(0, tok), pl.ds(h * HSUB, HSUB)],
                                    ysem.at[h])
        out.start()
        outs.append(out)
    for n in (4, 5):
        link(nh - 1, n).wait_send()
    for out in outs:
        out.wait()


def solution(mesh):
    ep_axes = tuple(mesh.axis_names)
    n_dev = math.prod(mesh.shape[a] for a in ep_axes)
    row_spec = P(ep_axes, None)
    w_spec = P(ep_axes, None, None)

    def local_layer(tokens, expert_ids, gate_weights, w_gate, w_up, w_down):
        tok, hidden = tokens.shape
        topk = expert_ids.shape[1]
        n_loc, _, ff = w_gate.shape
        per_exp = n_dev * tok * topk // (n_dev * n_loc)
        kc, hc = CSUB * 128, HSUB * 128
        nc, nh = hidden // kc, hidden // hc
        n_tok = n_dev * tok
        half = tok // 2
        acc_rows = max(2 * n_loc * per_exp * (ff // 128), (n_loc * per_exp + 8) * HSUB + nh * 8 * half * HSUB)
        dims = (tok, hidden, ff, n_loc, per_exp, topk)
        scratch = [
            [pltpu.VMEM((n_tok + 8, CSUB, 128), BF16) for _ in range(nc)],
            pltpu.VMEM((n_dev, topk, tok), jnp.int32),
            pltpu.VMEM((n_dev, topk, tok), F32),
            pltpu.VMEM((n_dev + 1, n_loc, tok), jnp.int32),
            pltpu.VMEM((n_dev + 1, n_loc, tok), F32),
            pltpu.VMEM((n_loc + 8, 256), jnp.int32),
            pltpu.VMEM((n_tok // 16, 128), jnp.int32),
            pltpu.VMEM((n_tok, 128), jnp.int32),
            pltpu.VMEM((n_loc, per_exp, 128), F32),
            pltpu.VMEM((8 * (per_exp + 8), 128), F32),
            pltpu.VMEM((per_exp, kc), BF16),
            pltpu.VMEM((acc_rows // 8, 8, 128), F32),
            pltpu.VMEM((n_loc, per_exp, ff), BF16),
            pltpu.VMEM((RING, max(3 * kc, ff), hc), BF16),
            pltpu.VMEM((nh, 8, half * HSUB, 128), BF16),
            pltpu.VMEM((nh, 8, half * HSUB, 128), BF16),
            pltpu.VMEM((nh, 7, half * HSUB, 128), BF16),
            pltpu.VMEM((nh, 6, half * HSUB, 128), BF16),
            pltpu.VMEM((tok + 1, hidden // 128, 128), BF16),
            pltpu.SMEM((n_loc, 256), jnp.int32),
            pltpu.SMEM((8, 128), jnp.int32),
            pltpu.SMEM((8, 128), jnp.int32),
            pltpu.VMEM((2, 8, 8, 128), jnp.int32),
            pltpu.SemaphoreType.DMA((nc,)),
            pltpu.SemaphoreType.DMA((4,)),
            pltpu.SemaphoreType.DMA((2, n_dev - 1)),
            pltpu.SemaphoreType.DMA((2, n_dev - 1)),
            pltpu.SemaphoreType.DMA((nc, 13)),
            pltpu.SemaphoreType.DMA((nc, 13)),
            pltpu.SemaphoreType.DMA((RING, 4)),
            pltpu.SemaphoreType.DMA((nh, 8)),
            pltpu.SemaphoreType.DMA((nh, 8)),
            pltpu.SemaphoreType.DMA((nh, 6)),
            pltpu.SemaphoreType.DMA((nh, 6)),
            pltpu.SemaphoreType.DMA((nh,)),
            pltpu.SemaphoreType.DMA((2,)),
        ]
        out = pl.pallas_call(
            functools.partial(moe_kernel, dims),
            out_shape=jax.ShapeDtypeStruct((tok, hidden // 128, 128), BF16),
            in_specs=[pl.BlockSpec(memory_space=pl.ANY)] * 6,
            out_specs=pl.BlockSpec(memory_space=pl.ANY),
            scratch_shapes=scratch,
            compiler_params=pltpu.CompilerParams(collective_id=0, has_side_effects=True,
                                                 vmem_limit_bytes=67043328),
        )(tokens, expert_ids.T, gate_weights.T, w_gate, w_up, w_down)
        return out.reshape(tok, hidden)

    return jax.shard_map(local_layer, mesh=mesh, in_specs=(row_spec, row_spec, row_spec, w_spec, w_spec, w_spec), out_specs=row_spec, check_vma=False)
```

```python
import functools
import math

import jax
import jax.numpy as jnp
from jax import lax
from jax.experimental import pallas as pl
from jax.experimental.pallas import tpu as pltpu
from jax.sharding import PartitionSpec as P

MESH = pl.DeviceIdType.MESH
F32 = jnp.float32
BF16 = jnp.bfloat16
RING = 5
CSUB = 4
HSUB = 8
TBLK = 64
TGRP = 4
UNROLL = 8


def unrolled(n, fn):
    def body(i, carry):
        fn(jnp.minimum(i, n - 1))
        return carry
    lax.fori_loop(0, n + 1, body, 0, unroll=n)


def moe_kernel(dims, x_hbm, ids_hbm, gts_hbm, w1_hbm, w3_hbm, w2_hbm, y_hbm,
               xall, ids_all, gts_all, chosen_pos, gate_tab, tok_tab, row_tab, pos_col, gcol, xg, xb, acc, hid, ring,
               psend, drecv, qsend, lrecv, ybuf, tok_sm, win_p, win_m, row_ord,
               loc_sem, tab_sem, rsend, rrecv, asend, arecv, wsem, dsend, drsem, lsend, lrsem, ysem, row_sem):
    tok, hidden, ff, n_loc, per_exp, topk = dims
    nc = hidden // (CSUB * 128)
    kc = CSUB * 128
    nh = hidden // (HSUB * 128)
    hc = HSUB * 128
    half = tok // 2
    n_dev = 8
    ct_ff = ff // 128
    zero_row = n_loc * per_exp
    xs = per_exp + 8

    z, y, c = lax.axis_index("ez"), lax.axis_index("ey"), lax.axis_index("ex")
    me = z * 4 + y * 2 + c
    xn, yn, pn = (z, 1 - y, c), (1 - z, y, c), (z, y, 1 - c)
    i_x = z * 4 + (1 - y) * 2 + c
    i_y = (1 - z) * 4 + y * 2 + c
    i_d = (1 - z) * 4 + (1 - y) * 2 + c

    def flip(i):
        b2, b1, b0 = (i >> 2) & 1, (i >> 1) & 1, i & 1
        t = (1 - z if b2 else z, 1 - y if b1 else y, 1 - c if b0 else c)
        return t, t[0] * 4 + t[1] * 2 + t[2]

    tail = ff - hc

    def w13_copies(k, e, slot):
        out = []
        for m, w in enumerate((w1_hbm, w3_hbm)):
            rows = pl.ds(k * kc, kc)
            out.append(pltpu.make_async_copy(w.at[e, rows, pl.ds(0, hc)], ring.at[slot, pl.ds(m * kc, kc), pl.ds(0, hc)], wsem.at[slot, 2 * m]))
            out.append(pltpu.make_async_copy(w.at[e, rows, pl.ds(hc, tail)], ring.at[slot, pl.ds(2 * kc, kc), pl.ds(m * tail, tail)],
                                             wsem.at[slot, 2 * m + 1]))
        return out

    def w2_copy(h, e, slot):
        return pltpu.make_async_copy(w2_hbm.at[e, :, pl.ds(pl.multiple_of(h * hc, hc), hc)], ring.at[slot, pl.ds(0, ff)],
                                     wsem.at[slot, 0])

    def weight(slot, m, ct, w):
        if ct * 128 < hc:
            return ring[slot, m * kc:(m + 1) * kc, ct * 128:(ct + w) * 128]
        c0 = m * tail + ct * 128 - hc
        return ring[slot, 2 * kc:3 * kc, c0:c0 + w * 128]

    own = pl.ds(pl.multiple_of(me * tok, tok), tok)
    loc = [pltpu.make_async_copy(x_hbm.at[pl.ds(0, tok), pl.ds(k * hc, hc)], ring.at[RING - 1, pl.ds(k * tok, tok)], loc_sem.at[k])
           for k in range(nh)]
    rlocs = [pltpu.make_async_copy(ids_hbm, ids_all.at[me], tab_sem.at[0]),
             pltpu.make_async_copy(gts_hbm, gts_all.at[me], tab_sem.at[3])]
    for cp in rlocs:
        cp.start()
    for cp in loc:
        cp.start()
    barrier = pltpu.get_barrier_semaphore()
    for i in range(1, n_dev):
        pl.semaphore_signal(barrier, inc=1, device_id=flip(i)[0], device_id_type=MESH)
    for e in range(RING - 1):
        for cp in w13_copies(0, e, e):
            cp.start()

    def own_rows(k):
        at = k * CSUB // HSUB
        for ct in range(CSUB):
            col = (k * CSUB + ct) % HSUB * 128
            xg[pl.ds(ct, tok, stride=CSUB), :] = ring[RING - 1, at * tok:(at + 1) * tok, col:col + 128].astype(F32)

        def one(t):
            xall[k][me * tok + t] = xg[pl.ds(pl.multiple_of(t * CSUB, CSUB), CSUB), :].astype(BF16)

        unrolled(tok, one)

    loc[0].wait()
    own_rows(0)
    pl.semaphore_wait(barrier, n_dev - 1)

    for cp in rlocs:
        cp.wait()
    rcopies = []
    for i in range(1, n_dev):
        for q, ref in enumerate((ids_all, gts_all)):
            cp = pltpu.make_async_remote_copy(ref.at[me], ref.at[me], rsend.at[q, i - 1], rrecv.at[q, i - 1],
                                              device_id=flip(i)[0], device_id_type=MESH)
            cp.start()
            rcopies.append(cp)

    def region(k, dev, lo, n):
        return xall[k].at[pl.ds(pl.multiple_of(dev * tok + lo, half), n)]

    partner_of = lambda d: d + 1 - 2 * c
    i_p = partner_of(me)
    flows = [
        (xn, me, i_x, 0, half), (xn, me, i_x, half, half), (xn, i_y, i_d, half, half),
        (yn, me, i_y, half, half), (yn, me, i_y, 0, half), (yn, i_x, i_d, 0, half),
        (pn, me, i_p, 0, tok),
        (pn, i_x, partner_of(i_x), 0, half), (pn, i_x, partner_of(i_x), half, half),
        (pn, i_y, partner_of(i_y), half, half), (pn, i_y, partner_of(i_y), 0, half),
        (pn, i_d, partner_of(i_d), 0, half), (pn, i_d, partner_of(i_d), half, half),
    ]

    def ag(k, n):
        tgt, src, _, lo, rows = flows[n]
        return pltpu.make_async_remote_copy(region(k, src, lo, rows), region(k, src, lo, rows),
                                            asend.at[k, n], arecv.at[k, n], device_id=tgt, device_id_type=MESH)

    def ag_recv(k, n):
        tgt, _, src, lo, rows = flows[n]
        pltpu.make_async_remote_copy(region(k, src, lo, rows), region(k, src, lo, rows),
                                     asend.at[k, n], arecv.at[k, n], device_id=tgt, device_id_type=MESH).wait_recv()

    def own_sends(k):
        for n in (0, 3, 1, 4, 6):
            ag(k, n).start()

    def relay1(k):
        ag_recv(k, 0)
        ag(k, 5).start()
        ag(k, 7).start()
        ag_recv(k, 3)
        ag(k, 2).start()
        ag(k, 9).start()

    def relay2(k):
        ag_recv(k, 1)
        ag(k, 8).start()
        ag_recv(k, 4)
        ag(k, 10).start()

    def relay3(k):
        ag_recv(k, 5)
        ag(k, 11).start()
        ag_recv(k, 2)
        ag(k, 12).start()

    def finish(k):
        for n in (6, 7, 9, 8, 10, 11, 12):
            ag_recv(k, n)

    own_sends(0)
    for k in range(1, nc):
        if k * CSUB % HSUB == 0:
            loc[k * CSUB // HSUB].wait()
        own_rows(k)
    for cp in w13_copies(0, RING - 1, RING - 1):
        cp.start()

    for cp in rcopies:
        cp.wait()
    base = me * n_loc
    my_ids = lax.broadcasted_iota(jnp.int32, (n_loc, tok), 0) + base
    off = jnp.zeros((n_loc, 1), jnp.int32)
    for s in range(n_dev):
        ids_s = ids_all[s]
        gts_s = gts_all[s]
        hit = jnp.zeros((n_loc, tok), jnp.int32)
        gden = jnp.zeros((n_loc, tok), F32)
        for j in range(topk):
            m = ids_s[j:j + 1, :] == my_ids
            hit = jnp.where(m, 1, hit)
            gden = gden + jnp.where(m, gts_s[j:j + 1, :], 0.0)
        cum = hit
        step = 1
        while step < tok:
            cum = cum + jnp.concatenate([jnp.zeros((n_loc, step), jnp.int32), cum[:, 0:tok - step]], axis=1)
            step *= 2
        pos = off + cum - 1
        off = off + cum[:, tok - 1:tok]
        posm = jnp.where(hit > 0, pos, -1)
        chosen_pos[s] = posm
        pos_col[s * tok:(s + 1) * tok, 0:n_loc] = posm.T
        gate_tab[s] = gden
        rows = jnp.full((topk, tok), zero_row, jnp.int32)
        for e in range(n_loc):
            rows = jnp.where(ids_s == base + e, e * per_exp + pos[e:e + 1, :], rows)
        for q in range(tok // 128):
            at = (s * (tok // 128) + q) * 8
            row_tab[at:at + topk, :] = rows[:, q * 128:(q + 1) * 128] * HSUB
            row_tab[at + topk:at + 8, :] = jnp.zeros((8 - topk, 128), jnp.int32)
    order = [(i_d, 0), (i_d, 1), (i_x, 0), (i_y, 1), (i_x, 1), (i_y, 0), (me, 0), (me, 1)]
    n_blk = len(order)
    for b, (dev, hf) in enumerate(order):
        for side, d in enumerate((partner_of(dev), dev)):
            row_ord[side, b] = row_tab[pl.ds(pl.multiple_of((d * 2 + hf) * 8, 8), 8), :]

    def window(side, b):
        return pltpu.make_async_copy(row_ord.at[side, b], (win_p, win_m)[side], row_sem.at[side])

    relay1(0)
    own_sends(1)
    relay2(0)
    lpos = lax.broadcasted_iota(jnp.int32, (TBLK, per_exp), 1)
    tcol = lax.broadcasted_iota(jnp.int32, (TBLK, per_exp), 0)
    for e0 in range(0, n_loc, TGRP):
        def tok_step(i, sums, e0=e0):
            pc = pos_col[pl.ds(pl.multiple_of(i * TBLK, TBLK), TBLK), :]
            out = []
            for e in range(TGRP):
                hitv = jnp.where(pc[:, e0 + e:e0 + e + 1] == lpos, tcol + i * TBLK, 0)
                out.append(sums[e] + jnp.sum(hitv.reshape(TBLK // 8, 8, per_exp), axis=0))
            return tuple(out)

        sums = lax.fori_loop(0, n_dev * tok // TBLK, tok_step,
                             tuple(jnp.zeros((8, per_exp), jnp.int32) for _ in range(TGRP)), unroll=4)
        for e in range(TGRP):
            tok_tab[e0 + e:e0 + e + 1, 0:per_exp] = jnp.sum(sums[e], axis=0, keepdims=True)

    tok_cp = pltpu.make_async_copy(tok_tab.at[0:n_loc], tok_sm, tab_sem.at[2])
    tok_cp.start()

    relay3(0)

    tok_cp.wait()
    finish(0)
    relay1(1)
    own_sends(2)

    def acc_row(e, mat, ct):
        return ((e * 2 + mat) * ct_ff + ct) * (per_exp // 8)

    def pick(k, e, lo, n):
        def one(i):
            xg[pl.ds(lo + i, CSUB, stride=xs), :] = xall[k][tok_sm[e, lo + i]].astype(F32)

        unrolled(n, one)

    def gate_column(e):
        ipos = lax.broadcasted_iota(jnp.int32, (per_exp, tok), 0)
        gsum = jnp.zeros((per_exp, tok), F32)
        for s in range(n_dev):
            prow = chosen_pos[s, pl.ds(e, 1), :]
            grow = gate_tab[s, pl.ds(e, 1), :]
            gsum = gsum + jnp.where(prow == ipos, grow, 0.0)
        gcol[e] = jnp.broadcast_to(jnp.sum(gsum, axis=1, keepdims=True), (per_exp, 128))

    def proj_step(k, e):
        slot = lax.rem(k * n_loc + e, RING)
        for cp in w13_copies(k, e, slot):
            cp.wait()
        for ct in range(CSUB):
            xb[:, ct * 128:(ct + 1) * 128] = xg[ct * xs:ct * xs + per_exp, :].astype(BF16)
        nxt = jnp.minimum(e + 1, n_loc - 1)
        if k == 1:
            gate_column(e)
        steps = list(range(0, ct_ff, 2))
        share = per_exp // len(steps)
        for si, ct in enumerate(steps):
            w = min(2, ct_ff - ct)
            if w == 2:
                d = [jnp.dot(xb[...], weight(slot, mat, ct, w), preferred_element_type=F32) for mat in range(2)]
            else:
                both = jnp.concatenate([weight(slot, mat, ct, w) for mat in range(2)], axis=1)
                r = jnp.dot(xb[...], both, preferred_element_type=F32)
                d = [r[:, 0:128], r[:, 128:256]]
            pick(k, nxt, si * share, share)
            for q in range(w):
                parts = []
                for mat in range(2):
                    at = pl.ds(acc_row(e, mat, ct + q), per_exp // 8)
                    v = d[mat][:, q * 128:(q + 1) * 128]
                    if k > 0:
                        v = v + acc[at].reshape(per_exp, 128)
                    if k < nc - 1:
                        acc[at] = v.reshape(per_exp // 8, 8, 128)
                    parts.append(v)
                if k == nc - 1:
                    hid[e, :, (ct + q) * 128:(ct + q + 1) * 128] = (jax.nn.silu(parts[0]) * parts[1]).astype(BF16)
        @pl.when(e < n_loc - RING)
        def _():
            for cp in w13_copies(k, e + RING, slot):
                cp.start()

        @pl.when(e >= n_loc - RING)
        def _():
            if k < nc - 1:
                for cp in w13_copies(k + 1, e + RING - n_loc, slot):
                    cp.start()
            else:
                w2_copy(0, e + RING - n_loc, slot).start()

    for k in range(nc):
        pick(k, 0, 0, per_exp)

        def body(e, carry, k=k):
            proj_step(k, e)
            if k + 1 < nc:
                if k > 0:
                    @pl.when(e == 0)
                    def _():
                        relay1(k + 1)
                        if k + 2 < nc:
                            own_sends(k + 2)

                @pl.when(e == (4 if k > 0 else 1))
                def _():
                    relay2(k + 1)

                @pl.when(e == 6)
                def _():
                    relay3(k + 1)
            return carry

        lax.fori_loop(0, n_loc, body, 0)
        if k + 1 < nc:
            finish(k + 1)

    flat = acc.reshape(acc.shape[0] * 8, 128)

    def down(h):
        def body(e, carry):
            step = h * n_loc + e
            slot = lax.rem(nc * n_loc + step, RING)
            w2_copy(h, e, slot).wait()
            g = gcol[e]
            for n in range(0, HSUB, 2):
                o = jnp.dot(hid[e], ring[slot, 0:ff, n * 128:(n + 2) * 128], preferred_element_type=F32)
                for q in range(2):
                    flat[pl.ds(e * (per_exp * HSUB) + n + q, per_exp, stride=HSUB), :] = o[:, q * 128:(q + 1) * 128] * g

            @pl.when(e < n_loc - RING)
            def _():
                w2_copy(h, e + RING, slot).start()

            @pl.when(jnp.logical_and(e >= n_loc - RING, h < nh - 1))
            def _():
                w2_copy(h + 1, e + RING - n_loc, slot).start()

            return carry

        lax.fori_loop(0, n_loc, body, 0)

    def pair_sum(win, i):
        out = []
        for t in (2 * i, 2 * i + 1):
            v = flat[pl.ds(win[0, t], HSUB), :]
            for j in range(1, topk):
                v = v + flat[pl.ds(win[j, t], HSUB), :]
            out.append(v)
        return jnp.concatenate(out, axis=0)

    pr = 2 * HSUB
    f_base = zero_row + 8

    def at_pair(i):
        return pl.ds(i * pr if isinstance(i, int) else pl.multiple_of(i * pr, pr), pr)

    def kept(h, b):
        return f_base + (h * n_blk + b) * half

    def d2d(h, b):
        return pltpu.make_async_remote_copy(psend.at[h, b], drecv.at[h, b], dsend.at[h, b], drsem.at[h, b],
                                            device_id=pn, device_id_type=MESH)

    def link(h, n):
        par = n % 2 if isinstance(n, int) else lax.rem(n, 2)
        tgt = (z + par * (1 - 2 * z), y + (1 - par) * (1 - 2 * y), c)
        return pltpu.make_async_remote_copy(qsend.at[h, n], lrecv.at[h, n], lsend.at[h, n], lrsem.at[h, n],
                                            device_id=tgt, device_id_type=MESH)

    def pairs(fn):
        def body(i, carry):
            for u in range(UNROLL):
                fn(i * UNROLL + u)
            return carry
        lax.fori_loop(0, half // (2 * UNROLL), body, 0)

    def relay_part(h, n, rn, base):
        link(h, rn).wait_recv()

        def fn(i):
            v = acc[pl.ds(base + i * 2, 2)].reshape(pr, 128)
            qsend[h, n, at_pair(i), :] = (v + lrecv[h, rn, at_pair(i), :].astype(F32)).astype(BF16)

        pairs(fn)
        link(h, n).start()

    def combine_relay(h):
        relay_part(h, 4, 1, kept(h, 4))
        relay_part(h, 5, 0, kept(h, 5))

    def combine_send(h):
        def body(b, carry):
            @pl.when(b < n_blk)
            def _():
                window(0, b).wait()

                def part(i):
                    psend[h, b, at_pair(i), :] = pair_sum(win_p, i).astype(BF16)

                unrolled(half // 2, part)
                d2d(h, b).start()

                @pl.when(b < n_blk - 1)
                def _():
                    window(0, b + 1).start()

            @pl.when(b > 0)
            def _():
                m = b - 1
                d2d(h, m).wait_recv()
                window(1, m).wait()
                n = jnp.minimum(m, 6)

                def whole(i):
                    v = pair_sum(win_m, i) + drecv[h, m, at_pair(i), :].astype(F32)
                    qsend[h, n, at_pair(i), :] = v.astype(BF16)
                    acc[pl.ds(kept(h, m) + i * 2, 2)] = v.reshape(2, HSUB, 128)

                unrolled(half // 2, whole)

                @pl.when(m < n_blk - 1)
                def _():
                    window(1, m + 1).start()

                @pl.when(m < 4)
                def _():
                    link(h, m).start()

                @pl.when(m == n_blk - 1)
                def _():
                    combine_relay(h)

            return carry

        lax.fori_loop(0, n_blk + 1, body, 0)

    def final(h):
        for n in (2, 3, 4, 5):
            link(h, n).wait_recv()
        for lo, n1, n2 in ((0, 2, 5), (half, 3, 4)):
            def fn(i, lo=lo, n1=n1, n2=n2):
                v = acc[pl.ds(kept(h, 6) + i * 2 + lo, 2)].reshape(pr, 128)
                v = v + lrecv[h, n1, at_pair(i), :].astype(F32) + lrecv[h, n2, at_pair(i), :].astype(F32)
                for q in range(2):
                    t = (i * 2 + q) + lo
                    xr = jnp.concatenate([xall[h * (HSUB // CSUB) + m][me * tok + t] for m in range(HSUB // CSUB)], axis=0).astype(F32)
                    ybuf[t, h * HSUB:(h + 1) * HSUB, :] = (v[q * HSUB:(q + 1) * HSUB, :] + xr).astype(BF16)

            pairs(fn)

    acc[zero_row] = jnp.zeros((HSUB, 128), F32)

    def half_step(h, carry):
        window(0, 0).start()
        window(1, 0).start()
        down(h)

        combine_send(h)
        return carry

    lax.fori_loop(0, nh, half_step, 0)
    for k in range(nc):
        for n in range(13):
            ag(k, n).wait_send()
    for h in range(nh):
        for b in range(n_blk):
            d2d(h, b).wait_send()
        for n in range(6):
            if h < nh - 1 or n < 4:
                link(h, n).wait_send()
    outs = []
    for h in range(nh):
        final(h)
        out = pltpu.make_async_copy(ybuf.at[pl.ds(0, tok), pl.ds(h * HSUB, HSUB)], y_hbm.at[pl.ds(0, tok), pl.ds(h * HSUB, HSUB)],
                                    ysem.at[h])
        out.start()
        outs.append(out)
    for n in (4, 5):
        link(nh - 1, n).wait_send()
    for out in outs:
        out.wait()


def solution(mesh):
    ep_axes = tuple(mesh.axis_names)
    n_dev = math.prod(mesh.shape[a] for a in ep_axes)
    row_spec = P(ep_axes, None)
    w_spec = P(ep_axes, None, None)

    def local_layer(tokens, expert_ids, gate_weights, w_gate, w_up, w_down):
        tok, hidden = tokens.shape
        topk = expert_ids.shape[1]
        n_loc, _, ff = w_gate.shape
        per_exp = n_dev * tok * topk // (n_dev * n_loc)
        kc, hc = CSUB * 128, HSUB * 128
        nc, nh = hidden // kc, hidden // hc
        n_tok = n_dev * tok
        half = tok // 2
        acc_rows = max(2 * n_loc * per_exp * (ff // 128), (n_loc * per_exp + 8) * HSUB + nh * 8 * half * HSUB)
        dims = (tok, hidden, ff, n_loc, per_exp, topk)
        scratch = [
            [pltpu.VMEM((n_tok + 8, CSUB, 128), BF16) for _ in range(nc)],
            pltpu.VMEM((n_dev, topk, tok), jnp.int32),
            pltpu.VMEM((n_dev, topk, tok), F32),
            pltpu.VMEM((n_dev + 1, n_loc, tok), jnp.int32),
            pltpu.VMEM((n_dev + 1, n_loc, tok), F32),
            pltpu.VMEM((n_loc + 8, 256), jnp.int32),
            pltpu.VMEM((n_tok // 16, 128), jnp.int32),
            pltpu.VMEM((n_tok, 128), jnp.int32),
            pltpu.VMEM((n_loc, per_exp, 128), F32),
            pltpu.VMEM((8 * (per_exp + 8), 128), F32),
            pltpu.VMEM((per_exp, kc), BF16),
            pltpu.VMEM((acc_rows // 8, 8, 128), F32),
            pltpu.VMEM((n_loc, per_exp, ff), BF16),
            pltpu.VMEM((RING, max(3 * kc, ff), hc), BF16),
            pltpu.VMEM((nh, 8, half * HSUB, 128), BF16),
            pltpu.VMEM((nh, 8, half * HSUB, 128), BF16),
            pltpu.VMEM((nh, 7, half * HSUB, 128), BF16),
            pltpu.VMEM((nh, 6, half * HSUB, 128), BF16),
            pltpu.VMEM((tok + 1, hidden // 128, 128), BF16),
            pltpu.SMEM((n_loc, 256), jnp.int32),
            pltpu.SMEM((8, 128), jnp.int32),
            pltpu.SMEM((8, 128), jnp.int32),
            pltpu.VMEM((2, 8, 8, 128), jnp.int32),
            pltpu.SemaphoreType.DMA((nc,)),
            pltpu.SemaphoreType.DMA((4,)),
            pltpu.SemaphoreType.DMA((2, n_dev - 1)),
            pltpu.SemaphoreType.DMA((2, n_dev - 1)),
            pltpu.SemaphoreType.DMA((nc, 13)),
            pltpu.SemaphoreType.DMA((nc, 13)),
            pltpu.SemaphoreType.DMA((RING, 4)),
            pltpu.SemaphoreType.DMA((nh, 8)),
            pltpu.SemaphoreType.DMA((nh, 8)),
            pltpu.SemaphoreType.DMA((nh, 6)),
            pltpu.SemaphoreType.DMA((nh, 6)),
            pltpu.SemaphoreType.DMA((nh,)),
            pltpu.SemaphoreType.DMA((2,)),
        ]
        out = pl.pallas_call(
            functools.partial(moe_kernel, dims),
            out_shape=jax.ShapeDtypeStruct((tok, hidden // 128, 128), BF16),
            in_specs=[pl.BlockSpec(memory_space=pl.ANY)] * 6,
            out_specs=pl.BlockSpec(memory_space=pl.ANY),
            scratch_shapes=scratch,
            compiler_params=pltpu.CompilerParams(collective_id=0, has_side_effects=True,
                                                 vmem_limit_bytes=67043328),
        )(tokens, expert_ids.T, gate_weights.T, w_gate, w_up, w_down)
        return out.reshape(tok, hidden)

    return jax.shard_map(local_layer, mesh=mesh, in_specs=(row_spec, row_spec, row_spec, w_spec, w_spec, w_spec), out_specs=row_spec, check_vma=False)
```
